512 devices in a mesh: seq: 32 (over y, x), dp: 16 (over z, core).
Axes of the slice: x: 4, y: 8, z: 8, core: 2. Of those that a mesh axis runs over, the one named last changes fastest.
Arguments:
- layer_input: bfloat16 [16, 8192, 2560], P('dp', 'seq'), may hold values from -14400 to 14400
- scan_input: bfloat16 [16, 8192, 2560], P('dp', 'seq'), may hold values from -0.75 to 0.75
- scan_cotangent: bfloat16 [16, 8192, 2560], P('dp', 'seq'), may hold values from -0.03125 to 0.03125
- step_size: float32 [16, 40, 8192], P('dp', None, 'seq'), may hold values from 0.5 to 2
- log_decay: float32 [16, 40, 8192], P('dp', None, 'seq'), may hold values from -2.25 to 0
- state_inputs: bfloat16 [16, 8192, 256], P('dp', 'seq'), may hold values from -4 to 4
- entry_state: bfloat16 [16, 32, 2560, 128], P('dp', 'seq'), may hold values from -8 to 8
Outputs:
- state_input_grad: bfloat16 [16, 8192, 256], P('dp', 'seq')
- weight_grad: float32 [2560, 256], P(('seq', 'dp'))
The draws below stay inside these ranges and needn't reach their ends.
All inputs are finite; a program needn't handle non-finite values. Where the reference program divides by a largest or mean magnitude, that divisor is 1e-20 or more.
Results may differ from the reference program's by a relative error of at most 0.013.
Values may be sent and summed in bfloat16 or wider, within the bound.
No kernel may reach another device: no remote copies, remote signals or barrier semaphores. Data moves between devices by JAX's collectives and lax.ppermute only.
A program may use at most 128 MiB of HBM per device.

```python
import math
import jax
import jax.numpy as jnp
from jax import lax

D = 2560
HEADS = 40
HEADP = 64
NSTATE = 128
STRETCH = 256
STRETCHES_DEV = 1
TOK_DEV = 256
LSEQ = 8192
SEQS = 16
CHANNELS = 2560
N_SEQ = 32
N_DP = 16


def draw_layer_input(key, part):
    keys = jax.random.split(key, 5)
    noise_part = jax.random.truncated_normal(keys[1], -4.0, 4.0, (SEQS, LSEQ, D), jnp.float32)
    row_top = 10.0
    element_offset = lax.broadcasted_iota(jnp.float32, (1, LSEQ, 1), 1) / LSEQ
    sequence = lax.broadcasted_iota(jnp.float32, (SEQS, 1, 1), 0) / max(SEQS - 1, 1)
    row_ramp = (1.0 + 2.0 * element_offset) * (1.0 + 2.0 * sequence)
    row_scale = jnp.exp(jax.random.uniform(keys[2], (SEQS, LSEQ, 1), jnp.float32, 0.0, jnp.log(row_top)))
    column_scale = jnp.exp(jax.random.uniform(keys[3], (1, 1, D), jnp.float32, 0.0, jnp.log(10.0)))
    owners = jax.random.permutation(keys[4], N_SEQ * N_DP)
    seq_index = lax.broadcasted_iota(jnp.int32, (SEQS, LSEQ), 1) // TOK_DEV
    group_index = lax.broadcasted_iota(jnp.int32, (SEQS, LSEQ), 0)
    target = owners[seq_index * N_DP + group_index]
    column_block = lax.broadcasted_iota(jnp.int32, (1, 1, D), 2) // (D // (N_SEQ * N_DP))
    spike = jnp.where(column_block == target[:, :, None], 4.0, 1.0)
    return (noise_part * row_ramp * row_scale * column_scale * spike).astype(jnp.bfloat16)


def draw_log_decay(key, part):
    keys = jax.random.split(key, 7)
    fast_share = 0.5
    quick = jax.random.uniform(keys[0], (1, HEADS, 1), jnp.float32) < fast_share
    fast_rate = jnp.exp(jax.random.uniform(keys[1], (1, HEADS, 1), jnp.float32, jnp.log(1.0 / 50.0), jnp.log(1.0 / 30.0)))
    slow_rate = jnp.exp(jax.random.uniform(keys[2], (1, HEADS, 1), jnp.float32, jnp.log(0.05), jnp.log(0.4))) / LSEQ
    forgetting_speeds = jnp.where(quick, fast_rate, slow_rate)
    accelerator_gain = jnp.exp(jax.random.uniform(keys[3], (SEQS, HEADS, N_SEQ), jnp.float32, jnp.log(0.5), jnp.log(2.0)))
    accelerator_gain = jnp.repeat(accelerator_gain, TOK_DEV, axis=2)
    element_gain = jnp.exp(jax.random.uniform(keys[4], (SEQS, HEADS, LSEQ), jnp.float32, jnp.log(0.5), jnp.log(2.0)))
    outlier_indices = jax.random.randint(keys[5], (SEQS, 1, 1, 3), 0, LSEQ)
    objective_numbers = jax.random.uniform(keys[6], (SEQS, HEADS, 1, 3), jnp.float32, jnp.log(0.5), jnp.log(0.8))
    element_offset = lax.broadcasted_iota(jnp.int32, (1, 1, LSEQ, 1), 2)
    outlier_clusters = jnp.sum(jnp.where(element_offset == outlier_indices, objective_numbers, 0.0), axis=3)
    return -(forgetting_speeds * accelerator_gain * element_gain) + outlier_clusters


def shard_levels(rng, dims, cuts, least, high):
    gain = 1.0
    for axis_at, blocks in cuts:
        heights = jax.random.uniform(jax.random.fold_in(jax.random.fold_in(rng, 6), axis_at), (blocks,), jnp.float32, least / len(cuts), high / len(cuts))
        gain = gain * jnp.repeat(jnp.exp(heights), dims[axis_at] // blocks).reshape((-1,) + (1,) * (len(dims) - 1 - axis_at))
    return gain


def gaussian(own_key, shape, scale, bound, shards=(), held_as=jnp.bfloat16):
    values = scale * jax.random.normal(own_key, shape, jnp.float32)
    if shards:
        values = values * shard_levels(own_key, shape, shards, -0.22, 0.18)
    return jnp.clip(values, -bound, bound).astype(held_as)


def setup_inputs(seed: int = 0) -> dict:
    seeds = jax.random.split(jax.random.key(seed), 8)
    return {
        "layer_input": draw_layer_input(jax.random.fold_in(seeds[7], 71), 0),
        "scan_input": gaussian(seeds[1], (SEQS, LSEQ, CHANNELS), HEADP ** -0.5, 0.75, ((0, 16), (1, 32))),
        "scan_cotangent": gaussian(seeds[2], (SEQS, LSEQ, CHANNELS), (TOK_DEV * N_SEQ * HEADS // 8) ** -0.5, 0.03125, ((0, 16), (1, 32))),
        "step_size": jnp.clip(jnp.exp(math.log(2.0) - 1.3862944 * jax.random.uniform(seeds[3], (SEQS, HEADS, LSEQ), jnp.float32) ** shard_levels(seeds[3], (SEQS, HEADS, LSEQ), ((0, 16), (2, 32)), -0.2, 0.2)), 0.5, 2.0),
        "log_decay": draw_log_decay(jax.random.fold_in(seeds[7], 71), 0),
        "state_inputs": gaussian(seeds[5], (SEQS, LSEQ, 2 * NSTATE), 1.0, 4.0, ((0, 16), (1, 32))),
        "entry_state": gaussian(seeds[6], (SEQS, N_SEQ, CHANNELS, NSTATE), 2.0, 8.0, ((0, 16), (1, 32))),
    }


epsilon = 1e-6


def silu_slope(value):
    sigma = jax.nn.sigmoid(value)
    return sigma * (1.0 + value * (1.0 - sigma))


def block_terms(pieces):
    inputs, cotangents, steps, cumulative, writes, reads = pieces
    later = lax.broadcasted_iota(jnp.int32, (STRETCH, STRETCH), 0) >= lax.broadcasted_iota(jnp.int32, (STRETCH, STRETCH), 1)
    scores = jnp.einsum("shp,thp->hst", cotangents.astype(jnp.float32), inputs.astype(jnp.float32))
    spread = jnp.where(later[None], cumulative[:, :, None] - cumulative[:, None, :], 0.0)
    decay = jnp.where(later[None], jnp.exp(spread), 0.0)
    mixing = lax.optimization_barrier((scores * decay * steps[:, None, :]).astype(jnp.bfloat16)).astype(jnp.float32)
    inner_write = jnp.einsum("hst,sn->tn", mixing, reads.astype(jnp.float32))
    inner_read = jnp.einsum("hst,tn->sn", mixing, writes.astype(jnp.float32))
    weighted_cot = (cotangents.astype(jnp.float32) * jnp.exp(cumulative).T[:, :, None]).astype(jnp.bfloat16)
    weighted_in = (inputs.astype(jnp.float32) * (steps * jnp.exp(cumulative[:, -1:] - cumulative)).T[:, :, None]).astype(jnp.bfloat16)
    return inner_write, inner_read, weighted_cot, weighted_in, jnp.exp(cumulative[:, -1])


def rounded(state):
    return lax.optimization_barrier(state.astype(jnp.bfloat16)).astype(jnp.float32)


def backward_step(state, pieces):
    weighted, reading, cot_part, total = pieces
    carried = jnp.einsum("bthp,bhpn->btn", weighted.astype(jnp.float32), rounded(state))
    local = jnp.einsum("bthp,btn->bhpn", cot_part.astype(jnp.float32), reading.astype(jnp.float32))
    return local + total[:, :, None, None] * state, carried


def reference(layer_input, scan_input, scan_cotangent, step_size, log_decay, state_inputs, entry_state):
    blocks = LSEQ // STRETCH
    count = SEQS * blocks
    inputs = scan_input.reshape(count, STRETCH, HEADS, HEADP)
    cotangents = scan_cotangent.reshape(count, STRETCH, HEADS, HEADP)
    steps = step_size.reshape(SEQS, HEADS, blocks, STRETCH).transpose(0, 2, 1, 3).reshape(count, HEADS, STRETCH)
    decays = log_decay.reshape(SEQS, HEADS, blocks, STRETCH).transpose(0, 2, 1, 3).reshape(count, HEADS, STRETCH)
    cumulative = jnp.cumsum(decays, axis=2)
    preact = state_inputs.astype(jnp.float32)
    activated = jax.nn.silu(preact).astype(jnp.bfloat16)
    writes = activated[:, :, :NSTATE].reshape(count, STRETCH, NSTATE)
    reads = activated[:, :, NSTATE:].reshape(count, STRETCH, NSTATE)
    inner_write, inner_read, weighted_cot, weighted_in, totals = lax.map(
        block_terms, (inputs, cotangents, steps, cumulative, writes, reads))

    def by_block(array):
        return jnp.swapaxes(array.reshape((SEQS, blocks) + array.shape[1:]), 0, 1)

    ordered_in = by_block(weighted_in)
    ordered_cot = by_block(weighted_cot)
    ordered_writes = by_block(writes)
    ordered_reads = by_block(reads)
    ordered_totals = by_block(totals)
    zero_state = jnp.zeros((SEQS, HEADS, HEADP, NSTATE), jnp.float32)
    ignored, carried_write = lax.scan(backward_step, zero_state,
                                      (ordered_in, ordered_reads, ordered_cot, ordered_totals), reverse=True)

    entries = entry_state.reshape(SEQS, N_SEQ, HEADS, HEADP, NSTATE)
    block_ids = jnp.arange(blocks, dtype=jnp.int32)

    def forward_step(state, pieces):
        cot_part, writing, weighted, total, block_id = pieces
        saved = lax.dynamic_index_in_dim(entries, (block_id // STRETCHES_DEV).astype(jnp.int32), 1, keepdims=False)
        state = jnp.where(block_id % STRETCHES_DEV == 0, saved.astype(jnp.float32), state)
        carried = jnp.einsum("bthp,bhpn->btn", cot_part.astype(jnp.float32), rounded(state))
        local = jnp.einsum("bthp,btn->bhpn", weighted.astype(jnp.float32), writing.astype(jnp.float32))
        return local + total[:, :, None, None] * state, carried

    ignored, carried_read = lax.scan(forward_step, zero_state,
                                     (ordered_cot, ordered_writes, ordered_in, ordered_totals, block_ids))

    def by_token(array):
        return jnp.swapaxes(array, 0, 1).reshape(SEQS, LSEQ, NSTATE)

    grad_write = inner_write.reshape(SEQS, LSEQ, NSTATE) + by_token(carried_write)
    grad_read = inner_read.reshape(SEQS, LSEQ, NSTATE) + by_token(carried_read)
    state_input_grad = (jnp.concatenate([grad_write, grad_read], axis=2) * silu_slope(preact)).astype(jnp.bfloat16)

    peaks = jnp.max(jnp.abs(layer_input), axis=(0, 1)).astype(jnp.float32)
    factor = 1.0 / (peaks + epsilon)

    def add_sequence(running, pieces):
        rows, grads = pieces
        quantized = (rows.astype(jnp.float32) * factor).astype(jnp.bfloat16)
        product = lax.dot_general(quantized, grads, (((0,), (0,)), ((), ())), preferred_element_type=jnp.float32)
        return running + product, None

    summed, ignored = lax.scan(add_sequence, jnp.zeros((D, 2 * NSTATE), jnp.float32), (layer_input, state_input_grad))
    return state_input_grad, summed
```

```python
import functools

import jax
import jax.numpy as jnp
from jax import lax
from jax.experimental import pallas as pl
from jax.experimental.pallas import tpu as pltpu
from jax.sharding import Mesh
from jax.sharding import PartitionSpec as P

SEQ = ("seq_0", "seq_1")
DP = ("dp_0", "dp_1")
SEQ_DP = SEQ + DP

epsilon = 1e-06
f32 = jnp.float32
bf16 = jnp.bfloat16


def silu_slope(value):
    sigma = jax.nn.sigmoid(value)
    return sigma * (1.0 + value * (1.0 - sigma))


def exchange(x, axes):
    return lax.all_to_all(x, axes, 0, 0, tiled=True)


def scan_body(bound_ref, got_ref, out_ref, peak_ref):
    blocks, _, states = got_ref.shape
    rows = out_ref.shape[1]
    first = lax.broadcasted_iota(jnp.int32, (rows, states), 0) < bound_ref[0]
    state = jnp.zeros((rows, states), f32)
    peak = jnp.zeros((1, states), f32)
    for k in reversed(range(blocks)):
        out_ref[k] = state.astype(bf16)
        extra = got_ref[k, rows : rows + 8, :].astype(f32)
        peak = jnp.maximum(peak, extra[4:5])
        total = jnp.where(first, extra[0:1] + extra[1:2], extra[2:3] + extra[3:4])
        state = got_ref[k, :rows, :].astype(f32) + total * state
    peak_ref[...] = peak


def scan_states(got, bound, rows):
    blocks, _, states = got.shape
    return pl.pallas_call(
        scan_body,
        in_specs=[
            pl.BlockSpec(memory_space=pltpu.SMEM),
            pl.BlockSpec(memory_space=pltpu.VMEM),
        ],
        out_specs=[
            pl.BlockSpec(memory_space=pltpu.VMEM),
            pl.BlockSpec(memory_space=pltpu.VMEM),
        ],
        out_shape=[
            jax.ShapeDtypeStruct((blocks, rows, states), bf16),
            jax.ShapeDtypeStruct((1, states), f32),
        ],
        name="scan_states",
    )(bound, got)


def on_device(
    layer_input, scan_input, scan_cotangent, step_size, log_decay, state_inputs, entry_state
):
    _, tokens, width = layer_input.shape
    heads = step_size.shape[1]
    channels = scan_input.shape[2]
    head_size = channels // heads
    states = state_inputs.shape[2] // 2
    n_y, n_x, n_z, n_c = (lax.axis_size(a) for a in SEQ_DP)
    n_seq = n_y * n_x
    n_dp = n_z * n_c
    slice_rows = channels // n_seq
    own_rows = width // (n_seq * n_dp)
    place = lax.axis_index("seq_0") * n_x + lax.axis_index("seq_1")

    rows_in = layer_input.reshape(tokens, width)
    inputs = scan_input.reshape(tokens, heads, head_size)
    cotangents = scan_cotangent.reshape(tokens, heads, head_size)
    steps = step_size.reshape(heads, tokens)
    cumulative = jnp.cumsum(log_decay.reshape(heads, tokens), axis=1)
    preact = state_inputs.reshape(tokens, 2 * states).astype(f32)
    activated = jax.nn.silu(preact).astype(bf16)
    writes = activated[:, :states]
    reads = activated[:, states:]

    weighted_cot = (cotangents * jnp.exp(cumulative).T[:, :, None]).astype(bf16)
    from_later = jnp.einsum("thp,tn->hpn", weighted_cot, reads, preferred_element_type=f32)
    totals = jnp.exp(cumulative[:, -1])
    local_peaks = jnp.max(jnp.abs(rows_in), axis=0)
    head0 = [slice_rows * d // head_size for d in range(n_seq)]
    head1 = [min(h + 1, heads - 1) for h in head0]
    ones = jnp.ones((1, states), f32)
    first_heads = jnp.stack([totals[h] for h in head0])
    second_heads = jnp.stack([totals[h] for h in head1])

    def two(values):
        high = lax.reduce_precision(values, 8, 7)
        return high[:, None, None] * ones, (values - high)[:, None, None] * ones

    peak_rows = jnp.pad(
        local_peaks.reshape(n_seq, slice_rows), ((0, 0), (0, states - slice_rows))
    )[:, None, :]
    extras = jnp.concatenate(
        [
            *two(first_heads),
            *two(second_heads),
            peak_rows.astype(f32),
            jnp.zeros((n_seq, 3, states), f32),
        ],
        axis=1,
    ).astype(bf16)
    sent = jnp.concatenate(
        [from_later.astype(bf16).reshape(n_seq, slice_rows, states), extras], axis=1
    )
    got = exchange(sent, SEQ)
    bound = (head_size - (place * slice_rows) % head_size).astype(jnp.int32).reshape(1)
    slices, seq_peaks = scan_states(got, bound, slice_rows)
    beyond = exchange(slices, SEQ).reshape(channels, states)

    later = lax.broadcasted_iota(jnp.int32, (tokens, tokens), 0) >= lax.broadcasted_iota(
        jnp.int32, (tokens, tokens), 1
    )
    scores = jnp.einsum("shp,thp->hst", cotangents, inputs, preferred_element_type=f32)
    spread = jnp.where(later[None], cumulative[:, :, None] - cumulative[:, None, :], 0.0)
    decay = jnp.where(later[None], jnp.exp(spread), 0.0)
    mixing = (scores * decay * steps[:, None, :]).astype(bf16)
    inner_write = jnp.einsum("hst,sn->tn", mixing, reads, preferred_element_type=f32)
    inner_read = jnp.einsum("hst,tn->sn", mixing, writes, preferred_element_type=f32)
    weighted_in = (
        inputs * (steps * jnp.exp(cumulative[:, -1:] - cumulative)).T[:, :, None]
    ).astype(bf16)
    carried_read = jnp.dot(
        weighted_cot.reshape(tokens, channels),
        entry_state.reshape(channels, states),
        preferred_element_type=f32,
    )
    slope = silu_slope(preact)
    grad_read = ((inner_read + carried_read) * slope[:, states:]).astype(bf16)

    carried_write = jnp.dot(
        weighted_in.reshape(tokens, channels), beyond, preferred_element_type=f32
    )
    grad_write = ((inner_write + carried_write) * slope[:, :states]).astype(bf16)
    state_input_grad = jnp.concatenate([grad_write, grad_read], axis=1)

    def product(grads):
        return lax.dot_general(
            rows_in, grads, (((0,), (0,)), ((), ())), preferred_element_type=f32
        ).astype(bf16)

    halves = jnp.stack([product(grad_write), product(grad_read)])
    half = exchange(halves, "dp_1").astype(f32).sum(axis=0).astype(bf16)
    by_x = half.reshape(n_y, n_x, slice_rows, states).transpose(1, 0, 2, 3)
    quarter = exchange(by_x, "seq_1").astype(f32).sum(axis=0).astype(bf16)
    pieces = quarter.reshape(n_y * n_dp, own_rows, states)
    peak_part = jnp.broadcast_to(seq_peaks.astype(bf16)[None], (n_y * n_dp, 1, states))
    pieces = jnp.concatenate(
        [pieces, peak_part, jnp.zeros((n_y * n_dp, 8 - own_rows - 1, states), bf16)], axis=1
    )
    arrived = exchange(pieces, ("seq_0",) + DP).astype(f32)
    arrived = arrived.reshape(n_y, n_z, n_c, 8, states)
    summed = arrived[..., :own_rows, :].sum(axis=(0, 1))
    own_y = lax.axis_index("seq_0")
    own_q = lax.axis_index("dp_0") * n_c + lax.axis_index("dp_1")
    peaks = lax.dynamic_index_in_dim(arrived[..., own_rows, :], own_y, 0, keepdims=False)
    peaks = jnp.max(peaks, axis=(0, 1))
    peaks = lax.dynamic_slice_in_dim(peaks, own_q * own_rows, own_rows)
    factor = 1.0 / (peaks + epsilon)
    weight_grad = summed.transpose(1, 0, 2).reshape(own_rows, n_c * states) * factor[:, None]
    return state_input_grad[None], weight_grad


def solution(mesh):
    torus = Mesh(mesh.devices.reshape(8, 4, 8, 2), SEQ_DP)
    placed = (
        P(DP, SEQ, None),
        P(DP, SEQ, None),
        P(DP, SEQ, None),
        P(DP, None, SEQ),
        P(DP, None, SEQ),
        P(DP, SEQ, None),
        P(DP, SEQ, None, None),
    )
    return jax.shard_map(
        on_device,
        mesh=torus,
        in_specs=placed,
        out_specs=(P(DP, SEQ, None), P(SEQ_DP, None)),
        check_vma=False,
    )
```

```python
import functools

import jax
import jax.numpy as jnp
from jax import lax
from jax.experimental import pallas as pl
from jax.experimental.pallas import tpu as pltpu
from jax.sharding import Mesh
from jax.sharding import PartitionSpec as P

SEQ = ("seq_0", "seq_1")
DP = ("dp_0", "dp_1")
SEQ_DP = SEQ + DP

epsilon = 1e-06
f32 = jnp.float32
bf16 = jnp.bfloat16


def silu_slope(value):
    sigma = jax.nn.sigmoid(value)
    return sigma * (1.0 + value * (1.0 - sigma))


def exchange(x, axes):
    return lax.all_to_all(x, axes, 0, 0, tiled=True)


def scan_body(bound_ref, got_ref, out_ref, peak_ref):
    blocks, _, states = got_ref.shape
    rows = out_ref.shape[1]
    first = lax.broadcasted_iota(jnp.int32, (rows, states), 0) < bound_ref[0]
    state = jnp.zeros((rows, states), f32)
    peak = jnp.zeros((1, states), f32)
    for k in reversed(range(blocks)):
        out_ref[k] = state.astype(bf16)
        extra = got_ref[k, rows : rows + 8, :].astype(f32)
        peak = jnp.maximum(peak, extra[4:5])
        total = jnp.where(first, extra[0:1] + extra[1:2], extra[2:3] + extra[3:4])
        state = got_ref[k, :rows, :].astype(f32) + total * state
    peak_ref[...] = peak


def scan_states(got, bound, rows):
    blocks, _, states = got.shape
    return pl.pallas_call(
        scan_body,
        in_specs=[
            pl.BlockSpec(memory_space=pltpu.SMEM),
            pl.BlockSpec(memory_space=pltpu.VMEM),
        ],
        out_specs=[
            pl.BlockSpec(memory_space=pltpu.VMEM),
            pl.BlockSpec(memory_space=pltpu.VMEM),
        ],
        out_shape=[
            jax.ShapeDtypeStruct((blocks, rows, states), bf16),
            jax.ShapeDtypeStruct((1, states), f32),
        ],
        name="scan_states",
    )(bound, got)


def summary_body(in_ref, cot_ref, decay_ref, pre_ref, sent_ref, cum_ref, reads_ref, spread_ref):
    step = pl.program_id(0)
    heads, tokens = decay_ref.shape
    chunks, rows_all, states = sent_ref.shape
    span = cot_ref.shape[1]
    rows = span // chunks
    head_size = span * pl.num_programs(0) // heads

    @pl.when(step == 0)
    def _():
        below = lax.broadcasted_iota(jnp.int32, (tokens, tokens), 0)
        above = lax.broadcasted_iota(jnp.int32, (tokens, tokens), 1)
        cum = jnp.dot(
            decay_ref[...],
            (below <= above).astype(f32),
            precision=lax.Precision.HIGHEST,
            preferred_element_type=f32,
        )
        cum_ref[...] = cum
        grown = jnp.exp(cum)
        high = grown.astype(bf16)
        spread_ref[0] = high
        spread_ref[1] = (grown - high.astype(f32)).astype(bf16)
        value = pre_ref[:, states:].astype(f32)
        reads_ref[...] = (value / (1.0 + jnp.exp(-value))).astype(bf16)

    owner = lax.broadcasted_iota(jnp.int32, (heads, span), 0) * head_size - step * span
    lane = lax.broadcasted_iota(jnp.int32, (heads, span), 1)
    hot = jnp.where((lane >= owner) & (lane < owner + head_size), 1.0, 0.0).astype(bf16)
    both = (((0,), (0,)), ((), ()))
    scale = lax.dot_general(spread_ref[0], hot, both, preferred_element_type=f32)
    scale += lax.dot_general(spread_ref[1], hot, both, preferred_element_type=f32)
    weighted = (cot_ref[...].astype(f32) * scale).astype(bf16)
    later = lax.dot_general(weighted, reads_ref[...], both, preferred_element_type=f32)
    later = later.astype(bf16)
    peak = jnp.max(jnp.abs(in_ref[...]).astype(f32), axis=0, keepdims=True)
    peak = jnp.broadcast_to(peak, (8, span))
    last = scale[tokens - 1 :, :]
    row = lax.broadcasted_iota(jnp.int32, (rows_all - rows, states), 0)
    for d in range(chunks):
        sent_ref[d, :rows, :] = later[d * rows : (d + 1) * rows]
        first = jnp.broadcast_to(last[:, d * rows : d * rows + 1], (8, states))
        second = jnp.broadcast_to(last[:, (d + 1) * rows - 1 : (d + 1) * rows], (8, states))
        first_high = first.astype(bf16).astype(f32)
        second_high = second.astype(bf16).astype(f32)
        turned = pltpu.roll(peak, span - d * rows, 1) if d else peak
        extra = jnp.where(row == 0, first_high, first - first_high)
        extra = jnp.where(row == 2, second_high, extra)
        extra = jnp.where(row == 3, second - second_high, extra)
        extra = jnp.where(row >= 4, turned[:, :states], extra)
        sent_ref[d, rows:, :] = extra.astype(bf16)


def summarize(rows_in, cots, decays, pre, n_seq, head_states):
    tokens, channels = cots.shape
    heads = decays.shape[0]
    states = head_states
    grid = 4
    span = channels // grid
    rows = channels // n_seq
    return pl.pallas_call(
        summary_body,
        grid=(grid,),
        in_specs=[
            pl.BlockSpec((tokens, span), lambda i: (0, i)),
            pl.BlockSpec((tokens, span), lambda i: (0, i)),
            pl.BlockSpec((heads, tokens), lambda i: (0, 0)),
            pl.BlockSpec((tokens, 2 * states), lambda i: (0, 0)),
        ],
        out_specs=[
            pl.BlockSpec((n_seq // grid, rows + 8, states), lambda i: (i, 0, 0)),
            pl.BlockSpec((heads, tokens), lambda i: (0, 0)),
        ],
        out_shape=[
            jax.ShapeDtypeStruct((n_seq, rows + 8, states), bf16),
            jax.ShapeDtypeStruct((heads, tokens), f32),
        ],
        scratch_shapes=[
            pltpu.VMEM((tokens, states), bf16),
            pltpu.VMEM((2, heads, tokens), bf16),
        ],
        name="summarize",
    )(rows_in, cots, decays, pre)


def finish_body(win_ref, beyond_ref, inner_ref, slope_ref, read_ref, turned_ref, peak_ref, grad_ref, prod_ref):
    states = beyond_ref.shape[1]
    half = turned_ref.shape[0] // 2
    carried = jnp.dot(win_ref[...], beyond_ref[...], preferred_element_type=f32)
    grad_ref[:, :states] = ((inner_ref[...] + carried) * slope_ref[...]).astype(bf16)
    grad_ref[:, states:] = read_ref[...]
    for c in range(2):
        prod_ref[c, :half, :] = jnp.dot(
            turned_ref[c * half : (c + 1) * half, :], grad_ref[...], preferred_element_type=f32
        ).astype(bf16)
        prod_ref[c, half:, :states] = jnp.broadcast_to(peak_ref[...], (8, states)).astype(bf16)
        prod_ref[c, half:, states:] = jnp.zeros((8, states), bf16)


def finish(weighted_in, beyond, inner, slope, grad_read, turned, peak):
    tokens = weighted_in.shape[0]
    width = turned.shape[0]
    states = beyond.shape[1]
    return pl.pallas_call(
        finish_body,
        out_shape=[
            jax.ShapeDtypeStruct((tokens, 2 * states), bf16),
            jax.ShapeDtypeStruct((2, width // 2 + 8, 2 * states), bf16),
        ],
        name="finish",
    )(weighted_in, beyond, inner, slope, grad_read, turned, peak)


def pair_body(got_ref, sum_ref, peak_ref):
    half = sum_ref.shape[0]
    sum_ref[...] = (got_ref[0, :half].astype(f32) + got_ref[1, :half].astype(f32)).astype(bf16)
    peak_ref[...] = jnp.maximum(got_ref[0, half:].astype(f32), got_ref[1, half:].astype(f32))


def add_pair(got):
    _, rows, cols = got.shape
    return pl.pallas_call(
        pair_body,
        out_shape=[
            jax.ShapeDtypeStruct((rows - 8, cols), bf16),
            jax.ShapeDtypeStruct((8, cols), f32),
        ],
        name="add_pair",
    )(got)


def split_body(got_ref, peak_ref, out_ref, sum_ref):
    count, rows, cols = got_ref.shape
    pieces = out_ref.shape[0]
    own = rows // pieces
    total = got_ref[0].astype(f32)
    for k in range(1, count):
        total += got_ref[k].astype(f32)
    sum_ref[:rows] = total
    sum_ref[rows:] = jnp.zeros((8, cols), f32)
    row = lax.broadcasted_iota(jnp.int32, (8, cols), 0)
    peak = peak_ref[...]
    for q in range(pieces):
        out_ref[q] = jnp.where(row < own, sum_ref[own * q : own * q + 8, :], peak).astype(bf16)


def add_split(got, peak, pieces):
    _, rows, cols = got.shape
    return pl.pallas_call(
        split_body,
        out_shape=jax.ShapeDtypeStruct((pieces, 8, cols), bf16),
        scratch_shapes=[pltpu.VMEM((rows + 8, cols), f32)],
        name="add_split",
    )(got, peak)


def close_body(place_ref, got_ref, out_ref):
    count, rows, cols = got_ref.shape
    own = out_ref.shape[0]
    total = got_ref[0].astype(f32)
    for k in range(1, count):
        total += got_ref[k].astype(f32)
    peak = jnp.zeros((rows, cols), f32)
    for z in range(8):
        peak = jnp.maximum(peak, got_ref[place_ref[0] * 8 + z].astype(f32))
    lane = lax.broadcasted_iota(jnp.int32, (rows, cols), 1)
    row = lax.broadcasted_iota(jnp.int32, (rows, cols), 0)
    line = jnp.broadcast_to(peak[own : own + 1, :], (rows, cols))
    column = jnp.sum(jnp.where(lane == place_ref[1] * own + row, line, 0.0), axis=1, keepdims=True)
    out_ref[...] = (total * (1.0 / (column + epsilon)))[:own]


def close(got, place, own):
    cols = got.shape[2]
    return pl.pallas_call(
        close_body,
        in_specs=[
            pl.BlockSpec(memory_space=pltpu.SMEM),
            pl.BlockSpec(memory_space=pltpu.VMEM),
        ],
        out_shape=jax.ShapeDtypeStruct((own, cols), f32),
        name="close",
    )(place, got)


def on_device(
    layer_input, scan_input, scan_cotangent, step_size, log_decay, state_inputs, entry_state
):
    _, tokens, width = layer_input.shape
    heads = step_size.shape[1]
    channels = scan_input.shape[2]
    head_size = channels // heads
    states = state_inputs.shape[2] // 2
    n_y, n_x, n_z, n_c = (lax.axis_size(a) for a in SEQ_DP)
    n_seq = n_y * n_x
    slice_rows = channels // n_seq
    own_rows = width // (n_seq * n_z * n_c)
    y, x, z, c = (lax.axis_index(a) for a in SEQ_DP)

    rows_in = layer_input.reshape(tokens, width)
    flat_cot = scan_cotangent.reshape(tokens, channels)
    flat_pre = state_inputs.reshape(tokens, 2 * states)
    sent, cumulative = summarize(
        rows_in, flat_cot, log_decay.reshape(heads, tokens), flat_pre, n_seq, states
    )
    got = exchange(sent, SEQ)
    bound = head_size - ((y * n_x + x) * slice_rows) % head_size
    slices, seq_peaks = scan_states(got, bound.astype(jnp.int32).reshape(1), slice_rows)
    beyond = exchange(slices, SEQ).reshape(channels, states)

    inputs = scan_input.reshape(tokens, heads, head_size)
    cotangents = scan_cotangent.reshape(tokens, heads, head_size)
    steps = step_size.reshape(heads, tokens)
    preact = flat_pre.astype(f32)
    activated = jax.nn.silu(preact).astype(bf16)
    writes = activated[:, :states]
    reads = activated[:, states:]
    weighted_cot = (cotangents * jnp.exp(cumulative).T[:, :, None]).astype(bf16)
    later = lax.broadcasted_iota(jnp.int32, (tokens, tokens), 0) >= lax.broadcasted_iota(
        jnp.int32, (tokens, tokens), 1
    )
    scores = jnp.einsum("shp,thp->hst", cotangents, inputs, preferred_element_type=f32)
    spread = jnp.where(later[None], cumulative[:, :, None] - cumulative[:, None, :], 0.0)
    decay = jnp.where(later[None], jnp.exp(spread), 0.0)
    mixing = (scores * decay * steps[:, None, :]).astype(bf16)
    inner_write = jnp.einsum("hst,sn->tn", mixing, reads, preferred_element_type=f32)
    inner_read = jnp.einsum("hst,tn->sn", mixing, writes, preferred_element_type=f32)
    weighted_in = (
        inputs * (steps * jnp.exp(cumulative[:, -1:] - cumulative)).T[:, :, None]
    ).astype(bf16)
    carried_read = jnp.dot(
        weighted_cot.reshape(tokens, channels),
        entry_state.reshape(channels, states),
        preferred_element_type=f32,
    )
    slope = silu_slope(preact)
    grad_read = ((inner_read + carried_read) * slope[:, states:]).astype(bf16)
    turned = rows_in.reshape(tokens, n_y, n_x, n_z, n_c, own_rows)
    turned = turned.transpose(4, 2, 1, 3, 5, 0).reshape(width, tokens)

    state_input_grad, product = finish(
        weighted_in.reshape(tokens, channels),
        beyond,
        inner_write,
        slope[:, :states],
        grad_read,
        turned,
        seq_peaks,
    )
    half, peaks = add_pair(exchange(product, "dp_1"))
    quarter = exchange(half.reshape(n_x, width // (n_x * n_c), 2 * states), "seq_1")
    pieces = add_split(quarter, peaks, n_y * n_z)
    arrived = exchange(pieces, ("seq_0", "dp_0"))
    where = jnp.stack([y, z * n_c + c]).astype(jnp.int32)
    return state_input_grad[None], close(arrived, where, own_rows)


def solution(mesh):
    torus = Mesh(mesh.devices.reshape(8, 4, 8, 2), SEQ_DP)
    placed = (
        P(DP, SEQ, None),
        P(DP, SEQ, None),
        P(DP, SEQ, None),
        P(DP, None, SEQ),
        P(DP, None, SEQ),
        P(DP, SEQ, None),
        P(DP, SEQ, None, None),
    )
    return jax.shard_map(
        on_device,
        mesh=torus,
        in_specs=placed,
        out_specs=(P(DP, SEQ, None), P(SEQ_DP, None)),
        check_vma=False,
    )
```

```python
import jax
import jax.numpy as jnp
from jax import lax
from jax.experimental import pallas as pl
from jax.experimental.pallas import tpu as pltpu
from jax.sharding import Mesh
from jax.sharding import PartitionSpec as P

SEQ = ("seq_0", "seq_1")
DP = ("dp_0", "dp_1")
SEQ_DP = SEQ + DP

epsilon = 1e-06
f32 = jnp.float32
bf16 = jnp.bfloat16


def budget(mib):
    return pltpu.CompilerParams(vmem_limit_bytes=mib * 2**20)


def exchange(x, axes):
    return lax.all_to_all(x, axes, 0, 0, tiled=True)


def scan_body(place_ref, got_ref, out_ref, peak_ref):
    blocks, _, states = got_ref.shape
    rows = out_ref.shape[1]
    first = lax.broadcasted_iota(jnp.int32, (rows, states), 0) < place_ref[2]
    state = jnp.zeros((rows, states), f32)
    peak = jnp.zeros((1, states), f32)
    for k in reversed(range(blocks)):
        out_ref[k] = state.astype(bf16)
        extra = got_ref[k, rows : rows + 8, :].astype(f32)
        peak = jnp.maximum(peak, extra[4:5])
        total = jnp.where(first, extra[0:1] + extra[1:2], extra[2:3] + extra[3:4])
        state = got_ref[k, :rows, :].astype(f32) + total * state
    peak_ref[...] = peak


def scan_states(got, place, rows):
    blocks, _, states = got.shape
    return pl.pallas_call(
        scan_body,
        in_specs=[
            pl.BlockSpec(memory_space=pltpu.SMEM),
            pl.BlockSpec(memory_space=pltpu.VMEM),
        ],
        out_specs=[
            pl.BlockSpec(memory_space=pltpu.VMEM),
            pl.BlockSpec(memory_space=pltpu.VMEM),
        ],
        out_shape=[
            jax.ShapeDtypeStruct((blocks, rows, states), bf16),
            jax.ShapeDtypeStruct((1, states), f32),
        ],
        compiler_params=budget(8),
        name="scan_states",
    )(place, got)


def summary_body(in_ref, cot_ref, decay_ref, pre_ref, sent_ref, reads_ref, spread_ref):
    step = pl.program_id(0)
    heads, tokens = decay_ref.shape
    chunks, rows_all, states = sent_ref.shape
    span = cot_ref.shape[1]
    rows = span // chunks
    head_size = span * pl.num_programs(0) // heads

    @pl.when(step == 0)
    def _():
        below = lax.broadcasted_iota(jnp.int32, (tokens, tokens), 0)
        above = lax.broadcasted_iota(jnp.int32, (tokens, tokens), 1)
        cum = jnp.dot(
            decay_ref[...],
            (below <= above).astype(f32),
            precision=lax.Precision.HIGHEST,
            preferred_element_type=f32,
        )
        grown = jnp.exp(cum)
        high = grown.astype(bf16)
        spread_ref[0] = high
        spread_ref[1] = (grown - high.astype(f32)).astype(bf16)
        value = pre_ref[:, states:].astype(f32)
        reads_ref[...] = (value / (1.0 + jnp.exp(-value))).astype(bf16)

    owner = lax.broadcasted_iota(jnp.int32, (heads, span), 0) * head_size - step * span
    lane = lax.broadcasted_iota(jnp.int32, (heads, span), 1)
    hot = jnp.where((lane >= owner) & (lane < owner + head_size), 1.0, 0.0).astype(bf16)
    both = (((0,), (0,)), ((), ()))
    scale = lax.dot_general(spread_ref[0], hot, both, preferred_element_type=f32)
    scale += lax.dot_general(spread_ref[1], hot, both, preferred_element_type=f32)
    weighted = (cot_ref[...].astype(f32) * scale).astype(bf16)
    later = lax.dot_general(weighted, reads_ref[...], both, preferred_element_type=f32)
    later = later.astype(bf16)
    peak = jnp.max(jnp.abs(in_ref[...]).astype(f32), axis=0, keepdims=True)
    peak = jnp.broadcast_to(peak, (8, span))
    last = scale[tokens - 1 :, :]
    row = lax.broadcasted_iota(jnp.int32, (rows_all - rows, states), 0)
    for d in range(chunks):
        sent_ref[d, :rows, :] = later[d * rows : (d + 1) * rows]
        first = jnp.broadcast_to(last[:, d * rows : d * rows + 1], (8, states))
        second = jnp.broadcast_to(last[:, (d + 1) * rows - 1 : (d + 1) * rows], (8, states))
        first_high = first.astype(bf16).astype(f32)
        second_high = second.astype(bf16).astype(f32)
        turned = pltpu.roll(peak, span - d * rows, 1) if d else peak
        extra = jnp.where(row == 0, first_high, first - first_high)
        extra = jnp.where(row == 2, second_high, extra)
        extra = jnp.where(row == 3, second - second_high, extra)
        extra = jnp.where(row >= 4, turned[:, :states], extra)
        sent_ref[d, rows:, :] = extra.astype(bf16)


def summarize(rows_in, cots, decays, pre, n_seq, head_states):
    tokens, channels = cots.shape
    heads = decays.shape[0]
    states = head_states
    grid = 4
    span = channels // grid
    rows = channels // n_seq
    return pl.pallas_call(
        summary_body,
        grid=(grid,),
        in_specs=[
            pl.BlockSpec((tokens, span), lambda i: (0, i)),
            pl.BlockSpec((tokens, span), lambda i: (0, i)),
            pl.BlockSpec((heads, tokens), lambda i: (0, 0)),
            pl.BlockSpec((tokens, 2 * states), lambda i: (0, 0)),
        ],
        out_specs=pl.BlockSpec((n_seq // grid, rows + 8, states), lambda i: (i, 0, 0)),
        out_shape=jax.ShapeDtypeStruct((n_seq, rows + 8, states), bf16),
        scratch_shapes=[
            pltpu.VMEM((tokens, states), bf16),
            pltpu.VMEM((2, heads, tokens), bf16),
        ],
        compiler_params=budget(60),
        name="summarize",
    )(rows_in, cots, decays, pre)


def inner_body(
    cot_ref,
    in_ref,
    decay_ref,
    step_ref,
    pre_ref,
    entry_ref,
    win_ref,
    inner_ref,
    slope_ref,
    read_ref,
    column_ref,
    row_ref,
    spread_ref,
    mix_ref,
    carry_ref,
):
    step = pl.program_id(0)
    heads, tokens = decay_ref.shape
    span = cot_ref.shape[1]
    states = entry_ref.shape[1]
    per_step = heads // pl.num_programs(0)
    head_size = span // per_step
    half = tokens // 2
    both = (((0,), (0,)), ((), ()))
    last = (((1,), (1,)), ((), ()))

    @pl.when(step == 0)
    def _():
        one = lax.broadcasted_iota(jnp.int32, (tokens, tokens), 0)
        two = lax.broadcasted_iota(jnp.int32, (tokens, tokens), 1)
        cum = jnp.dot(
            decay_ref[...],
            (one <= two).astype(f32),
            precision=lax.Precision.HIGHEST,
            preferred_element_type=f32,
        )
        column_ref[...] = jnp.zeros_like(column_ref)
        column_ref[:, :heads] = lax.dot_general(
            (one >= two).astype(f32),
            decay_ref[...],
            last,
            precision=lax.Precision.HIGHEST,
            preferred_element_type=f32,
        )
        row_ref[...] = cum - jnp.log(step_ref[...])
        grown = jnp.exp(cum)
        shrunk = jnp.exp(cum[:, tokens - 1 :] - cum) * step_ref[...]
        for k, value in enumerate((grown, shrunk)):
            high = value.astype(bf16)
            spread_ref[2 * k] = high
            spread_ref[2 * k + 1] = (value - high.astype(f32)).astype(bf16)
        mix_ref[...] = jnp.zeros_like(mix_ref)
        carry_ref[...] = jnp.zeros_like(carry_ref)

    owner = lax.broadcasted_iota(jnp.int32, (heads, span), 0) * head_size - step * span
    lane = lax.broadcasted_iota(jnp.int32, (heads, span), 1)
    hot = jnp.where((lane >= owner) & (lane < owner + head_size), 1.0, 0.0).astype(bf16)

    def expanded(k):
        scale = lax.dot_general(spread_ref[2 * k], hot, both, preferred_element_type=f32)
        return scale + lax.dot_general(
            spread_ref[2 * k + 1], hot, both, preferred_element_type=f32
        )

    win_ref[...] = (in_ref[...].astype(f32) * expanded(1)).astype(bf16)
    weighted_cot = (cot_ref[...].astype(f32) * expanded(0)).astype(bf16)
    carry_ref[...] += jnp.dot(weighted_cot, entry_ref[...], preferred_element_type=f32)

    columns = pltpu.roll(column_ref[...], lax.rem(128 - per_step * step, 128), 1)
    rows = [row_ref[pl.ds(per_step * step + j, 1), :] for j in range(per_step)]
    low = lax.broadcasted_iota(jnp.int32, (half, 2 * head_size), 1) < head_size
    later = lax.broadcasted_iota(jnp.int32, (half, half), 0) >= lax.broadcasted_iota(
        jnp.int32, (half, half), 1
    )
    for s, t in ((0, 0), (1, 0), (1, 1)):
        total = mix_ref[s * half : (s + 1) * half, t * half : (t + 1) * half]
        for j in range(per_step):
            lanes = slice(j // 2 * 2 * head_size, (j // 2 + 1) * 2 * head_size)
            left = cot_ref[s * half : (s + 1) * half, lanes]
            keep = low if j % 2 == 0 else jnp.logical_not(low)
            left = jnp.where(keep, left.astype(f32), 0.0).astype(bf16)
            right = in_ref[t * half : (t + 1) * half, lanes]
            scores = lax.dot_general(left, right, last, preferred_element_type=f32)
            gap = columns[s * half : (s + 1) * half, j : j + 1] - rows[j][
                :, t * half : (t + 1) * half
            ]
            if s == t:
                gap = jnp.where(later, gap, -1e30)
            total += scores * jnp.exp(gap)
        mix_ref[s * half : (s + 1) * half, t * half : (t + 1) * half] = total

    @pl.when(step == pl.num_programs(0) - 1)
    def _():
        value = pre_ref[...].astype(f32)
        sigma = 1.0 / (1.0 + jnp.exp(-value))
        active = (value / (1.0 + jnp.exp(-value))).astype(bf16)
        slope = sigma * (1.0 + value * (1.0 - sigma))
        mixed = mix_ref[...].astype(bf16)
        inner_ref[...] = lax.dot_general(
            mixed, active[:, states:], both, preferred_element_type=f32
        )
        read = carry_ref[...] + jnp.dot(mixed, active[:, :states], preferred_element_type=f32)
        slope_ref[...] = slope[:, :states]
        read_ref[...] = (read * slope[:, states:]).astype(bf16)


def inner_terms(cots, ins, decays, steps, pre, entry):
    tokens, channels = cots.shape
    heads = decays.shape[0]
    states = entry.shape[1]
    grid = 4
    span = channels // grid
    whole = lambda i: (0, 0)
    return pl.pallas_call(
        inner_body,
        grid=(grid,),
        in_specs=[
            pl.BlockSpec((tokens, span), lambda i: (0, i)),
            pl.BlockSpec((tokens, span), lambda i: (0, i)),
            pl.BlockSpec((heads, tokens), whole),
            pl.BlockSpec((heads, tokens), whole),
            pl.BlockSpec((tokens, 2 * states), whole),
            pl.BlockSpec((span, states), lambda i: (i, 0)),
        ],
        out_specs=[
            pl.BlockSpec((tokens, span), lambda i: (0, i)),
            pl.BlockSpec((tokens, states), whole),
            pl.BlockSpec((tokens, states), whole),
            pl.BlockSpec((tokens, states), whole),
        ],
        out_shape=[
            jax.ShapeDtypeStruct((tokens, channels), bf16),
            jax.ShapeDtypeStruct((tokens, states), f32),
            jax.ShapeDtypeStruct((tokens, states), f32),
            jax.ShapeDtypeStruct((tokens, states), bf16),
        ],
        scratch_shapes=[
            pltpu.VMEM((tokens, 128), f32),
            pltpu.VMEM((heads, tokens), f32),
            pltpu.VMEM((4, heads, tokens), bf16),
            pltpu.VMEM((tokens, tokens), f32),
            pltpu.VMEM((tokens, states), f32),
        ],
        compiler_params=budget(16),
        cost_estimate=pl.CostEstimate(
            flops=4 * 10**9, transcendentals=2 * 10**6, bytes_accessed=6 * 10**6
        ),
        name="inner_terms",
    )(cots, ins, decays, steps, pre, entry)


def turn_body(in_ref, out_ref, hot_ref):
    n_c, n_x, _, part, _ = out_ref.shape
    span = in_ref.shape[1]
    n_z, own = 8, part // 16

    @pl.when(pl.program_id(0) == 0)
    def _():
        row = lax.broadcasted_iota(jnp.int32, (span, 1), 0)
        i, row = lax.rem(row, own), lax.div(row, own)
        z, row = lax.rem(row, n_z), lax.div(row, n_z)
        y, row = lax.rem(row, 2), lax.div(row, 2)
        x, c = lax.rem(row, n_x), lax.div(row, n_x)
        source = (((y * n_x + x) * n_z + z) * n_c + c) * own + i
        lane = lax.broadcasted_iota(jnp.int32, (span, span), 1)
        hot_ref[...] = jnp.where(lane == source, 1.0, 0.0).astype(bf16)

    turned = lax.dot_general(
        hot_ref[...], in_ref[...], (((1,), (1,)), ((), ())), preferred_element_type=f32
    ).astype(bf16)
    for c in range(n_c):
        for x in range(n_x):
            at = (c * n_x + x) * part
            out_ref[c, x, 0] = turned[at : at + part]


def turn(rows_in, n_x, n_c):
    tokens, width = rows_in.shape
    grid = 4
    span = width // grid
    part = span // (n_x * n_c)
    return pl.pallas_call(
        turn_body,
        grid=(grid,),
        in_specs=[pl.BlockSpec((tokens, span), lambda i: (0, i))],
        out_specs=pl.BlockSpec((n_c, n_x, 1, part, tokens), lambda i: (0, 0, i, 0, 0)),
        out_shape=jax.ShapeDtypeStruct((n_c, n_x, grid, part, tokens), bf16),
        scratch_shapes=[pltpu.VMEM((span, span), bf16)],
        compiler_params=budget(12),
        cost_estimate=pl.CostEstimate(
            flops=10**9, transcendentals=0, bytes_accessed=3 * 10**6
        ),
        name="turn",
    )(rows_in).reshape(width, tokens)


def finish_body(win_ref, beyond_ref, inner_ref, slope_ref, read_ref, turned_ref, peak_ref, grad_ref, prod_ref):
    states = beyond_ref.shape[1]
    half = turned_ref.shape[0] // 2
    carried = jnp.dot(win_ref[...], beyond_ref[...], preferred_element_type=f32)
    grad_ref[:, :states] = ((inner_ref[...] + carried) * slope_ref[...]).astype(bf16)
    grad_ref[:, states:] = read_ref[...]
    for c in range(2):
        prod_ref[c, :half, :] = jnp.dot(
            turned_ref[c * half : (c + 1) * half, :], grad_ref[...], preferred_element_type=f32
        ).astype(bf16)
        prod_ref[c, half:, :states] = jnp.broadcast_to(peak_ref[...], (8, states)).astype(bf16)
        prod_ref[c, half:, states:] = jnp.zeros((8, states), bf16)


def finish(weighted_in, beyond, inner, slope, grad_read, turned, peak):
    tokens = weighted_in.shape[0]
    width = turned.shape[0]
    states = beyond.shape[1]
    return pl.pallas_call(
        finish_body,
        out_shape=[
            jax.ShapeDtypeStruct((tokens, 2 * states), bf16),
            jax.ShapeDtypeStruct((2, width // 2 + 8, 2 * states), bf16),
        ],
        compiler_params=budget(16),
        name="finish",
    )(weighted_in, beyond, inner, slope, grad_read, turned, peak)


def pair_body(got_ref, sum_ref, peak_ref):
    half = sum_ref.shape[0]
    sum_ref[...] = (got_ref[0, :half].astype(f32) + got_ref[1, :half].astype(f32)).astype(bf16)
    peak_ref[...] = jnp.maximum(got_ref[0, half:].astype(f32), got_ref[1, half:].astype(f32))


def add_pair(got):
    _, rows, cols = got.shape
    return pl.pallas_call(
        pair_body,
        out_shape=[
            jax.ShapeDtypeStruct((rows - 8, cols), bf16),
            jax.ShapeDtypeStruct((8, cols), f32),
        ],
        compiler_params=budget(8),
        name="add_pair",
    )(got)


def split_body(got_ref, peak_ref, out_ref, sum_ref):
    count, rows, cols = got_ref.shape
    pieces = out_ref.shape[0]
    own = rows // pieces
    total = got_ref[0].astype(f32)
    for k in range(1, count):
        total += got_ref[k].astype(f32)
    sum_ref[:rows] = total
    sum_ref[rows:] = jnp.zeros((8, cols), f32)
    row = lax.broadcasted_iota(jnp.int32, (8, cols), 0)
    peak = peak_ref[...]
    for q in range(pieces):
        out_ref[q] = jnp.where(row < own, sum_ref[own * q : own * q + 8, :], peak).astype(bf16)


def add_split(got, peak, pieces):
    _, rows, cols = got.shape
    return pl.pallas_call(
        split_body,
        out_shape=jax.ShapeDtypeStruct((pieces, 8, cols), bf16),
        scratch_shapes=[pltpu.VMEM((rows + 8, cols), f32)],
        compiler_params=budget(6),
        name="add_split",
    )(got, peak)


def close_body(place_ref, got_ref, out_ref):
    count, rows, cols = got_ref.shape
    own = out_ref.shape[0]
    total = got_ref[0].astype(f32)
    for k in range(1, count):
        total += got_ref[k].astype(f32)
    peak = jnp.zeros((rows, cols), f32)
    for z in range(8):
        peak = jnp.maximum(peak, got_ref[place_ref[0] * 8 + z].astype(f32))
    lane = lax.broadcasted_iota(jnp.int32, (rows, cols), 1)
    row = lax.broadcasted_iota(jnp.int32, (rows, cols), 0)
    line = jnp.broadcast_to(peak[own : own + 1, :], (rows, cols))
    column = jnp.sum(jnp.where(lane == place_ref[1] * own + row, line, 0.0), axis=1, keepdims=True)
    out_ref[...] = (total * (1.0 / (column + epsilon)))[:own]


def close(got, place, own):
    cols = got.shape[2]
    return pl.pallas_call(
        close_body,
        in_specs=[
            pl.BlockSpec(memory_space=pltpu.SMEM),
            pl.BlockSpec(memory_space=pltpu.VMEM),
        ],
        out_shape=jax.ShapeDtypeStruct((own, cols), f32),
        compiler_params=budget(4),
        name="close",
    )(place, got)


def on_device(
    layer_input, scan_input, scan_cotangent, step_size, log_decay, state_inputs, entry_state
):
    _, tokens, width = layer_input.shape
    heads = step_size.shape[1]
    channels = scan_input.shape[2]
    head_size = channels // heads
    states = state_inputs.shape[2] // 2
    n_y, n_x, n_z, n_c = (lax.axis_size(a) for a in SEQ_DP)
    n_seq = n_y * n_x
    slice_rows = channels // n_seq
    own_rows = width // (n_seq * n_z * n_c)
    y, x, z, c = (lax.axis_index(a) for a in SEQ_DP)

    rows_in = layer_input.reshape(tokens, width)
    flat_cot = scan_cotangent.reshape(tokens, channels)
    flat_pre = state_inputs.reshape(tokens, 2 * states)
    decays = log_decay.reshape(heads, tokens)
    sent = summarize(rows_in, flat_cot, decays, flat_pre, n_seq, states)
    got = exchange(sent, SEQ)
    bound = head_size - ((y * n_x + x) * slice_rows) % head_size
    place = jnp.stack([y, z * n_c + c, bound]).astype(jnp.int32)
    slices, seq_peaks = scan_states(got, place, slice_rows)
    beyond = exchange(slices, SEQ).reshape(channels, states)

    weighted_in, inner_write, slope, grad_read = inner_terms(
        flat_cot,
        scan_input.reshape(tokens, channels),
        decays,
        step_size.reshape(heads, tokens),
        flat_pre,
        entry_state.reshape(channels, states),
    )
    turned = turn(rows_in, n_x, n_c)
    state_input_grad, product = finish(
        weighted_in, beyond, inner_write, slope, grad_read, turned, seq_peaks
    )
    half, peaks = add_pair(exchange(product, "dp_1"))
    quarter = exchange(half.reshape(n_x, width // (n_x * n_c), 2 * states), "seq_1")
    pieces = add_split(quarter, peaks, n_y * n_z)
    arrived = exchange(pieces, ("seq_0", "dp_0"))
    return state_input_grad[None], close(arrived, place, own_rows)


def solution(mesh):
    torus = Mesh(mesh.devices.reshape(8, 4, 8, 2), SEQ_DP)
    placed = (
        P(DP, SEQ, None),
        P(DP, SEQ, None),
        P(DP, SEQ, None),
        P(DP, None, SEQ),
        P(DP, None, SEQ),
        P(DP, SEQ, None),
        P(DP, SEQ, None, None),
    )
    return jax.shard_map(
        on_device,
        mesh=torus,
        in_specs=placed,
        out_specs=(P(DP, SEQ, None), P(SEQ_DP, None)),
        check_vma=False,
    )
```

```python
import jax
import jax.numpy as jnp
from jax import lax
from jax.experimental import pallas as pl
from jax.experimental.pallas import tpu as pltpu
from jax.sharding import Mesh
from jax.sharding import PartitionSpec as P

SEQ = ("seq_0", "seq_1")
DP = ("dp_0", "dp_1")
SEQ_DP = SEQ + DP

epsilon = 1e-06
f32 = jnp.float32
bf16 = jnp.bfloat16


def silu_slope(value):
    sigma = 1.0 / (1.0 + jnp.exp(-value))
    return sigma * (1.0 + value * (1.0 - sigma))


def budget(mib):
    return pltpu.CompilerParams(vmem_limit_bytes=mib * 2**20)


def exchange(x, axes):
    return lax.all_to_all(x, axes, 0, 0, tiled=True)


def scan_body(place_ref, got_ref, out_ref, peak_ref):
    blocks, _, states = got_ref.shape
    rows = out_ref.shape[1]
    first = lax.broadcasted_iota(jnp.int32, (rows, states), 0) < place_ref[2]
    state = jnp.zeros((rows, states), f32)
    peak = jnp.zeros((1, states), f32)
    for k in reversed(range(blocks)):
        out_ref[k] = state.astype(bf16)
        extra = got_ref[k, rows : rows + 8, :].astype(f32)
        peak = jnp.maximum(peak, extra[4:5])
        total = jnp.where(first, extra[0:1] + extra[1:2], extra[2:3] + extra[3:4])
        state = got_ref[k, :rows, :].astype(f32) + total * state
    peak_ref[...] = peak


def scan_states(got, place, rows):
    blocks, _, states = got.shape
    return pl.pallas_call(
        scan_body,
        in_specs=[
            pl.BlockSpec(memory_space=pltpu.SMEM),
            pl.BlockSpec(memory_space=pltpu.VMEM),
        ],
        out_specs=[
            pl.BlockSpec(memory_space=pltpu.VMEM),
            pl.BlockSpec(memory_space=pltpu.VMEM),
        ],
        out_shape=[
            pltpu.VMEM((blocks, rows, states), bf16),
            jax.ShapeDtypeStruct((1, states), f32),
        ],
        compiler_params=budget(8),
        name="scan_states",
    )(place, got)


def summary_body(place_ref, in_ref, cot_ref, decay_ref, pre_ref, sent_ref, reads_ref, spread_ref):
    step = pl.program_id(0)
    heads, tokens = decay_ref.shape
    total, rows_all, states = sent_ref.shape
    chunks = total // pl.num_programs(0)
    span = cot_ref.shape[1]
    rows = span // chunks
    head_size = span * pl.num_programs(0) // heads

    @pl.when(step == 0)
    def _():
        below = lax.broadcasted_iota(jnp.int32, (tokens, tokens), 0)
        above = lax.broadcasted_iota(jnp.int32, (tokens, tokens), 1)
        cum = jnp.dot(
            decay_ref[...],
            (below <= above).astype(f32),
            precision=lax.Precision.HIGHEST,
            preferred_element_type=f32,
        )
        grown = jnp.exp(cum)
        high = grown.astype(bf16)
        spread_ref[0] = high
        spread_ref[1] = (grown - high.astype(f32)).astype(bf16)
        value = pre_ref[:, states:].astype(f32)
        reads_ref[...] = (value / (1.0 + jnp.exp(-value))).astype(bf16)

    owner = lax.broadcasted_iota(jnp.int32, (heads, span), 0) * head_size - step * span
    lane = lax.broadcasted_iota(jnp.int32, (heads, span), 1)
    hot = jnp.where((lane >= owner) & (lane < owner + head_size), 1.0, 0.0).astype(bf16)
    both = (((0,), (0,)), ((), ()))
    scale = lax.dot_general(spread_ref[0], hot, both, preferred_element_type=f32)
    scale += lax.dot_general(spread_ref[1], hot, both, preferred_element_type=f32)
    weighted = (cot_ref[...].astype(f32) * scale).astype(bf16)
    later = lax.dot_general(weighted, reads_ref[...], both, preferred_element_type=f32)
    later = later.astype(bf16)
    peak = jnp.max(jnp.abs(in_ref[...]).astype(f32), axis=0, keepdims=True)
    peak = jnp.broadcast_to(peak, (8, span))
    last = scale[tokens - 1 :, :]
    row = lax.broadcasted_iota(jnp.int32, (rows_all - rows, states), 0)
    for d in range(chunks):
        sent_ref[step * chunks + d, :rows, :] = later[d * rows : (d + 1) * rows]
        first = jnp.broadcast_to(last[:, d * rows : d * rows + 1], (8, states))
        second = jnp.broadcast_to(last[:, (d + 1) * rows - 1 : (d + 1) * rows], (8, states))
        first_high = first.astype(bf16).astype(f32)
        second_high = second.astype(bf16).astype(f32)
        turned = pltpu.roll(peak, span - d * rows, 1) if d else peak
        extra = jnp.where(row == 0, first_high, first - first_high)
        extra = jnp.where(row == 2, second_high, extra)
        extra = jnp.where(row == 3, second - second_high, extra)
        extra = jnp.where(row >= 4, turned[:, :states], extra)
        sent_ref[step * chunks + d, rows:, :] = extra.astype(bf16)


def summarize(place, rows_in, cots, decays, pre, n_seq, head_states):
    tokens, channels = cots.shape
    heads = decays.shape[0]
    states = head_states
    grid = 2
    span = channels // grid
    rows = channels // n_seq
    return pl.pallas_call(
        summary_body,
        grid=(grid,),
        in_specs=[
            pl.BlockSpec(memory_space=pltpu.SMEM),
            pl.BlockSpec((tokens, span), lambda i: (0, i)),
            pl.BlockSpec((tokens, span), lambda i: (0, i)),
            pl.BlockSpec((heads, tokens), lambda i: (0, 0)),
            pl.BlockSpec((tokens, 2 * states), lambda i: (0, 0)),
        ],
        out_specs=pl.BlockSpec(memory_space=pltpu.VMEM),
        out_shape=pltpu.VMEM((n_seq, rows + 8, states), bf16),
        scratch_shapes=[
            pltpu.VMEM((tokens, states), bf16),
            pltpu.VMEM((2, heads, tokens), bf16),
        ],
        compiler_params=budget(60),
        name="summarize",
    )(place, rows_in, cots, decays, pre)


def inner_body(
    cot_ref,
    in_ref,
    decay_ref,
    step_ref,
    pre_ref,
    entry_ref,
    out_ref,
    column_ref,
    row_ref,
    spread_ref,
    mix_ref,
    carry_ref,
):
    step = pl.program_id(0)
    heads, tokens = decay_ref.shape
    span = cot_ref.shape[1]
    states = entry_ref.shape[1]
    per_step = heads // pl.num_programs(0)
    head_size = span // per_step
    half = tokens // 2
    both = (((0,), (0,)), ((), ()))
    last = (((1,), (1,)), ((), ()))

    @pl.when(step == 0)
    def _():
        one = lax.broadcasted_iota(jnp.int32, (tokens, tokens), 0)
        two = lax.broadcasted_iota(jnp.int32, (tokens, tokens), 1)
        cum = jnp.dot(
            decay_ref[...],
            (one <= two).astype(f32),
            precision=lax.Precision.HIGHEST,
            preferred_element_type=f32,
        )
        column_ref[...] = jnp.zeros_like(column_ref)
        column_ref[:, :heads] = lax.dot_general(
            (one >= two).astype(f32),
            decay_ref[...],
            last,
            precision=lax.Precision.HIGHEST,
            preferred_element_type=f32,
        )
        row_ref[...] = cum - jnp.log(step_ref[...])
        grown = jnp.exp(cum)
        shrunk = jnp.exp(cum[:, tokens - 1 :] - cum) * step_ref[...]
        for k, value in enumerate((grown, shrunk)):
            high = value.astype(bf16)
            spread_ref[2 * k] = high
            spread_ref[2 * k + 1] = (value - high.astype(f32)).astype(bf16)
        mix_ref[...] = jnp.zeros_like(mix_ref)
        carry_ref[...] = jnp.zeros_like(carry_ref)

    owner = lax.broadcasted_iota(jnp.int32, (heads, span), 0) * head_size - step * span
    lane = lax.broadcasted_iota(jnp.int32, (heads, span), 1)
    hot = jnp.where((lane >= owner) & (lane < owner + head_size), 1.0, 0.0).astype(bf16)

    def expanded(k):
        scale = lax.dot_general(spread_ref[2 * k], hot, both, preferred_element_type=f32)
        return scale + lax.dot_general(
            spread_ref[2 * k + 1], hot, both, preferred_element_type=f32
        )

    at = pl.multiple_of(step * span, 128)
    out_ref[:, pl.ds(at, span)] = (in_ref[...].astype(f32) * expanded(1)).astype(bf16)
    weighted_cot = (cot_ref[...].astype(f32) * expanded(0)).astype(bf16)
    carry_ref[...] += jnp.dot(weighted_cot, entry_ref[...], preferred_element_type=f32)

    columns = pltpu.roll(column_ref[...], lax.rem(128 - per_step * step, 128), 1)
    rows = [row_ref[pl.ds(per_step * step + j, 1), :] for j in range(per_step)]
    low = lax.broadcasted_iota(jnp.int32, (half, 2 * head_size), 1) < head_size
    later = lax.broadcasted_iota(jnp.int32, (half, half), 0) >= lax.broadcasted_iota(
        jnp.int32, (half, half), 1
    )
    for s, t in ((0, 0), (1, 0), (1, 1)):
        total = mix_ref[s * half : (s + 1) * half, t * half : (t + 1) * half]
        for j in range(per_step):
            lanes = slice(j // 2 * 2 * head_size, (j // 2 + 1) * 2 * head_size)
            left = cot_ref[s * half : (s + 1) * half, lanes]
            keep = low if j % 2 == 0 else jnp.logical_not(low)
            left = jnp.where(keep, left.astype(f32), 0.0).astype(bf16)
            right = in_ref[t * half : (t + 1) * half, lanes]
            scores = lax.dot_general(left, right, last, preferred_element_type=f32)
            gap = columns[s * half : (s + 1) * half, j : j + 1] - rows[j][
                :, t * half : (t + 1) * half
            ]
            if s == t:
                gap = jnp.where(later, gap, -1e30)
            total += scores * jnp.exp(gap)
        mix_ref[s * half : (s + 1) * half, t * half : (t + 1) * half] = total

    @pl.when(step == pl.num_programs(0) - 1)
    def _():
        value = pre_ref[...].astype(f32)
        active = (value / (1.0 + jnp.exp(-value))).astype(bf16)
        mixed = mix_ref[...].astype(bf16)
        inner = lax.dot_general(mixed, active[:, states:], both, preferred_element_type=f32)
        high = inner.astype(bf16)
        channels = out_ref.shape[1] - 3 * states
        out_ref[:, channels : channels + states] = high
        low_part = (inner - high.astype(f32)).astype(bf16)
        out_ref[:, channels + states : channels + 2 * states] = low_part
        read = carry_ref[...] + jnp.dot(mixed, active[:, :states], preferred_element_type=f32)
        read = read * silu_slope(value[:, states:])
        out_ref[:, channels + 2 * states :] = read.astype(bf16)


def inner_terms(cots, ins, decays, steps, pre, entry):
    tokens, channels = cots.shape
    heads = decays.shape[0]
    states = entry.shape[1]
    grid = 4
    span = channels // grid
    whole = lambda i: (0, 0)
    return pl.pallas_call(
        inner_body,
        grid=(grid,),
        in_specs=[
            pl.BlockSpec((tokens, span), lambda i: (0, i)),
            pl.BlockSpec((tokens, span), lambda i: (0, i)),
            pl.BlockSpec((heads, tokens), whole),
            pl.BlockSpec((heads, tokens), whole),
            pl.BlockSpec((tokens, 2 * states), whole),
            pl.BlockSpec((span, states), lambda i: (i, 0)),
        ],
        out_specs=pl.BlockSpec(memory_space=pltpu.VMEM),
        out_shape=pltpu.VMEM((tokens, channels + 3 * states), bf16),
        scratch_shapes=[
            pltpu.VMEM((tokens, 128), f32),
            pltpu.VMEM((heads, tokens), f32),
            pltpu.VMEM((4, heads, tokens), bf16),
            pltpu.VMEM((tokens, tokens), f32),
            pltpu.VMEM((tokens, states), f32),
        ],
        compiler_params=budget(16),
        cost_estimate=pl.CostEstimate(
            flops=4 * 10**9, transcendentals=2 * 10**6, bytes_accessed=6 * 10**6
        ),
        name="inner_terms",
    )(cots, ins, decays, steps, pre, entry)


def turn_body(in_ref, out_ref, hot_ref):
    n_c, n_x, _, part, _ = out_ref.shape
    span = in_ref.shape[1]
    n_z, own = 8, part // 16

    @pl.when(pl.program_id(0) == 0)
    def _():
        row = lax.broadcasted_iota(jnp.int32, (span, 1), 0)
        i, row = lax.rem(row, own), lax.div(row, own)
        z, row = lax.rem(row, n_z), lax.div(row, n_z)
        y, row = lax.rem(row, 2), lax.div(row, 2)
        x, c = lax.rem(row, n_x), lax.div(row, n_x)
        source = (((y * n_x + x) * n_z + z) * n_c + c) * own + i
        lane = lax.broadcasted_iota(jnp.int32, (span, span), 1)
        hot_ref[...] = jnp.where(lane == source, 1.0, 0.0).astype(bf16)

    turned = lax.dot_general(
        hot_ref[...], in_ref[...], (((1,), (1,)), ((), ())), preferred_element_type=f32
    ).astype(bf16)
    for c in range(n_c):
        for x in range(n_x):
            at = (c * n_x + x) * part
            out_ref[c, x, 0] = turned[at : at + part]


def turn(rows_in, n_x, n_c):
    tokens, width = rows_in.shape
    grid = 4
    span = width // grid
    part = span // (n_x * n_c)
    return pl.pallas_call(
        turn_body,
        grid=(grid,),
        in_specs=[pl.BlockSpec((tokens, span), lambda i: (0, i))],
        out_specs=pl.BlockSpec((n_c, n_x, 1, part, tokens), lambda i: (0, 0, i, 0, 0)),
        out_shape=pltpu.VMEM((n_c, n_x, grid, part, tokens), bf16),
        scratch_shapes=[pltpu.VMEM((span, span), bf16)],
        compiler_params=budget(12),
        cost_estimate=pl.CostEstimate(
            flops=10**9, transcendentals=0, bytes_accessed=3 * 10**6
        ),
        name="turn",
    )(rows_in).reshape(width, tokens)


def finish_body(
    terms_ref, beyond_ref, pre_ref, turned_ref, peak_ref, grad_ref, prod_ref
):
    states = beyond_ref.shape[1]
    half = turned_ref.shape[0] // 2
    channels = beyond_ref.shape[0]
    carried = jnp.dot(terms_ref[:, :channels], beyond_ref[...], preferred_element_type=f32)
    inner = terms_ref[:, channels : channels + states].astype(f32)
    inner += terms_ref[:, channels + states : channels + 2 * states].astype(f32)
    grad = (inner + carried) * silu_slope(pre_ref[:, :states].astype(f32))
    grad_ref[:, :states] = grad.astype(bf16)
    grad_ref[:, states:] = terms_ref[:, channels + 2 * states :]
    for c in range(2):
        prod_ref[c, :half, :] = jnp.dot(
            turned_ref[c * half : (c + 1) * half, :], grad_ref[...], preferred_element_type=f32
        ).astype(bf16)
        prod_ref[c, half:, :states] = jnp.broadcast_to(peak_ref[...], (8, states)).astype(bf16)
        prod_ref[c, half:, states:] = jnp.zeros((8, states), bf16)


def finish(terms, beyond, pre, turned, peak):
    tokens = terms.shape[0]
    width = turned.shape[0]
    states = beyond.shape[1]
    return pl.pallas_call(
        finish_body,
        out_shape=[
            jax.ShapeDtypeStruct((tokens, 2 * states), bf16),
            jax.ShapeDtypeStruct((2, width // 2 + 8, 2 * states), bf16),
        ],
        compiler_params=budget(16),
        name="finish",
    )(terms, beyond, pre, turned, peak)


def pair_body(got_ref, sum_ref, peak_ref):
    half = sum_ref.shape[0]
    sum_ref[...] = (got_ref[0, :half].astype(f32) + got_ref[1, :half].astype(f32)).astype(bf16)
    peak_ref[...] = jnp.maximum(got_ref[0, half:].astype(f32), got_ref[1, half:].astype(f32))


def add_pair(got):
    _, rows, cols = got.shape
    return pl.pallas_call(
        pair_body,
        out_shape=[
            jax.ShapeDtypeStruct((rows - 8, cols), bf16),
            jax.ShapeDtypeStruct((8, cols), f32),
        ],
        compiler_params=budget(8),
        name="add_pair",
    )(got)


def split_body(got_ref, peak_ref, out_ref, sum_ref):
    count, rows, cols = got_ref.shape
    pieces = out_ref.shape[0]
    own = rows // pieces
    total = got_ref[0].astype(f32)
    for k in range(1, count):
        total += got_ref[k].astype(f32)
    sum_ref[:rows] = total
    sum_ref[rows:] = jnp.zeros((8, cols), f32)
    row = lax.broadcasted_iota(jnp.int32, (8, cols), 0)
    peak = peak_ref[...]
    for q in range(pieces):
        out_ref[q] = jnp.where(row < own, sum_ref[own * q : own * q + 8, :], peak).astype(bf16)


def add_split(got, peak, pieces):
    _, rows, cols = got.shape
    return pl.pallas_call(
        split_body,
        out_shape=jax.ShapeDtypeStruct((pieces, 8, cols), bf16),
        scratch_shapes=[pltpu.VMEM((rows + 8, cols), f32)],
        compiler_params=budget(6),
        name="add_split",
    )(got, peak)


def close_body(place_ref, got_ref, out_ref):
    count, rows, cols = got_ref.shape
    own = out_ref.shape[0]
    total = got_ref[0].astype(f32)
    for k in range(1, count):
        total += got_ref[k].astype(f32)
    peak = jnp.zeros((rows, cols), f32)
    for z in range(8):
        peak = jnp.maximum(peak, got_ref[place_ref[0] * 8 + z].astype(f32))
    lane = lax.broadcasted_iota(jnp.int32, (rows, cols), 1)
    row = lax.broadcasted_iota(jnp.int32, (rows, cols), 0)
    line = jnp.broadcast_to(peak[own : own + 1, :], (rows, cols))
    column = jnp.sum(jnp.where(lane == place_ref[1] * own + row, line, 0.0), axis=1, keepdims=True)
    out_ref[...] = (total * (1.0 / (column + epsilon)))[:own]


def close(got, place, own):
    cols = got.shape[2]
    return pl.pallas_call(
        close_body,
        in_specs=[
            pl.BlockSpec(memory_space=pltpu.SMEM),
            pl.BlockSpec(memory_space=pltpu.VMEM),
        ],
        out_shape=jax.ShapeDtypeStruct((own, cols), f32),
        compiler_params=budget(4),
        name="close",
    )(place, got)


def on_device(
    layer_input, scan_input, scan_cotangent, step_size, log_decay, state_inputs, entry_state
):
    _, tokens, width = layer_input.shape
    heads = step_size.shape[1]
    channels = scan_input.shape[2]
    head_size = channels // heads
    states = state_inputs.shape[2] // 2
    n_y, n_x, n_z, n_c = (lax.axis_size(a) for a in SEQ_DP)
    n_seq = n_y * n_x
    slice_rows = channels // n_seq
    own_rows = width // (n_seq * n_z * n_c)
    y, x, z, c = (lax.axis_index(a) for a in SEQ_DP)

    bound = head_size - ((y * n_x + x) * slice_rows) % head_size
    place = jnp.stack([y, z * n_c + c, bound]).astype(jnp.int32)
    rows_in = layer_input.reshape(tokens, width)
    flat_cot = scan_cotangent.reshape(tokens, channels)
    flat_pre = state_inputs.reshape(tokens, 2 * states)
    decays = log_decay.reshape(heads, tokens)
    sent = summarize(place, rows_in, flat_cot, decays, flat_pre, n_seq, states)
    got = exchange(sent, SEQ)
    slices, seq_peaks = scan_states(got, place, slice_rows)
    beyond = exchange(slices, SEQ).reshape(channels, states)

    terms = inner_terms(
        flat_cot,
        scan_input.reshape(tokens, channels),
        decays,
        step_size.reshape(heads, tokens),
        flat_pre,
        entry_state.reshape(channels, states),
    )
    turned = turn(rows_in, n_x, n_c)
    state_input_grad, product = finish(terms, beyond, flat_pre, turned, seq_peaks)
    half, peaks = add_pair(exchange(product, "dp_1"))
    quarter = exchange(half.reshape(n_x, width // (n_x * n_c), 2 * states), "seq_1")
    pieces = add_split(quarter, peaks, n_y * n_z)
    arrived = exchange(pieces, ("seq_0", "dp_0"))
    return state_input_grad[None], close(arrived, place, own_rows)


def solution(mesh):
    torus = Mesh(mesh.devices.reshape(8, 4, 8, 2), SEQ_DP)
    placed = (
        P(DP, SEQ, None),
        P(DP, SEQ, None),
        P(DP, SEQ, None),
        P(DP, None, SEQ),
        P(DP, None, SEQ),
        P(DP, SEQ, None),
        P(DP, SEQ, None, None),
    )
    return jax.shard_map(
        on_device,
        mesh=torus,
        in_specs=placed,
        out_specs=(P(DP, SEQ, None), P(SEQ_DP, None)),
        check_vma=False,
    )
```

```python
import functools

import jax
import jax.numpy as jnp
from jax import lax
from jax.experimental import pallas as pl
from jax.experimental.pallas import tpu as pltpu
from jax.sharding import Mesh
from jax.sharding import PartitionSpec as P

SEQ = ("seq_0", "seq_1")
DP = ("dp_0", "dp_1")
SEQ_DP = SEQ + DP

epsilon = 1e-06
f32 = jnp.float32
bf16 = jnp.bfloat16


def silu_slope(value):
    sigma = 1.0 / (1.0 + jnp.exp(-value))
    return sigma * (1.0 + value * (1.0 - sigma))


def budget(mib):
    return pltpu.CompilerParams(vmem_limit_bytes=mib * 2**20)


def exchange(x, axes):
    return lax.all_to_all(x, axes, 0, 0, tiled=True)


def swapped(x):
    return lax.ppermute(x, "dp_1", [(0, 1), (1, 0)])


def scan_body(head_size, got_ref, out_ref, peak_ref):
    blocks, _, states = got_ref.shape
    rows = out_ref.shape[1]
    slot = lax.axis_index("seq_0") * lax.axis_size("seq_1") + lax.axis_index("seq_1")
    bound = head_size - lax.rem(slot * rows, head_size)
    first = lax.broadcasted_iota(jnp.int32, (rows, states), 0) < bound
    state = jnp.zeros((rows, states), f32)
    peak = jnp.zeros((1, states), f32)
    for k in reversed(range(blocks)):
        out_ref[k] = state.astype(bf16)
        extra = got_ref[k, rows : rows + 8, :].astype(f32)
        peak = jnp.maximum(peak, extra[4:5])
        total = jnp.where(first, extra[0:1] + extra[1:2], extra[2:3] + extra[3:4])
        state = got_ref[k, :rows, :].astype(f32) + total * state
    peak_ref[...] = peak


def scan_states(got, rows, head_size):
    blocks, _, states = got.shape
    return pl.pallas_call(
        functools.partial(scan_body, head_size),
        out_shape=[
            pltpu.VMEM((blocks, rows, states), bf16),
            jax.ShapeDtypeStruct((1, states), f32),
        ],
        compiler_params=budget(8),
        name="scan_states",
    )(got)


def summary_body(in_ref, cot_ref, decay_ref, pre_ref, sent_ref, reads_ref, spread_ref):
    step = pl.program_id(0)
    heads, tokens = decay_ref.shape
    total, rows_all, states = sent_ref.shape
    chunks = total // pl.num_programs(0)
    span = cot_ref.shape[1]
    rows = span // chunks
    head_size = span * pl.num_programs(0) // heads

    @pl.when(step == 0)
    def _():
        below = lax.broadcasted_iota(jnp.int32, (tokens, tokens), 0)
        above = lax.broadcasted_iota(jnp.int32, (tokens, tokens), 1)
        cum = jnp.dot(
            decay_ref[...],
            (below <= above).astype(f32),
            precision=lax.Precision.HIGHEST,
            preferred_element_type=f32,
        )
        grown = jnp.exp(cum)
        high = grown.astype(bf16)
        spread_ref[0] = high
        spread_ref[1] = (grown - high.astype(f32)).astype(bf16)
        value = pre_ref[:, states:].astype(f32)
        reads_ref[...] = (value / (1.0 + jnp.exp(-value))).astype(bf16)

    owner = lax.broadcasted_iota(jnp.int32, (heads, span), 0) * head_size - step * span
    lane = lax.broadcasted_iota(jnp.int32, (heads, span), 1)
    hot = jnp.where((lane >= owner) & (lane < owner + head_size), 1.0, 0.0).astype(bf16)
    both = (((0,), (0,)), ((), ()))
    scale = lax.dot_general(spread_ref[0], hot, both, preferred_element_type=f32)
    scale += lax.dot_general(spread_ref[1], hot, both, preferred_element_type=f32)
    weighted = (cot_ref[...].astype(f32) * scale).astype(bf16)
    later = lax.dot_general(weighted, reads_ref[...], both, preferred_element_type=f32)
    later = later.astype(bf16)
    peak = jnp.max(jnp.abs(in_ref[...]).astype(f32), axis=0, keepdims=True)
    peak = jnp.broadcast_to(peak, (8, span))
    last = scale[tokens - 1 :, :]
    row = lax.broadcasted_iota(jnp.int32, (rows_all - rows, states), 0)
    for d in range(chunks):
        sent_ref[step * chunks + d, :rows, :] = later[d * rows : (d + 1) * rows]
        first = jnp.broadcast_to(last[:, d * rows : d * rows + 1], (8, states))
        second = jnp.broadcast_to(last[:, (d + 1) * rows - 1 : (d + 1) * rows], (8, states))
        first_high = first.astype(bf16).astype(f32)
        second_high = second.astype(bf16).astype(f32)
        turned = pltpu.roll(peak, span - d * rows, 1) if d else peak
        extra = jnp.where(row == 0, first_high, first - first_high)
        extra = jnp.where(row == 2, second_high, extra)
        extra = jnp.where(row == 3, second - second_high, extra)
        extra = jnp.where(row >= 4, turned[:, :states], extra)
        sent_ref[step * chunks + d, rows:, :] = extra.astype(bf16)


def summarize(rows_in, cots, decays, pre, n_seq, head_states):
    tokens, channels = cots.shape
    heads = decays.shape[0]
    states = head_states
    grid = 2
    span = channels // grid
    rows = channels // n_seq
    return pl.pallas_call(
        summary_body,
        grid=(grid,),
        in_specs=[
            pl.BlockSpec((tokens, span), lambda i: (0, i)),
            pl.BlockSpec((tokens, span), lambda i: (0, i)),
            pl.BlockSpec((heads, tokens), lambda i: (0, 0)),
            pl.BlockSpec((tokens, 2 * states), lambda i: (0, 0)),
        ],
        out_specs=pl.BlockSpec(memory_space=pltpu.VMEM),
        out_shape=pltpu.VMEM((n_seq, rows + 8, states), bf16),
        scratch_shapes=[
            pltpu.VMEM((tokens, states), bf16),
            pltpu.VMEM((2, heads, tokens), bf16),
        ],
        compiler_params=budget(60),
        name="summarize",
    )(rows_in, cots, decays, pre)


def inner_body(
    cot_ref,
    in_ref,
    decay_ref,
    step_ref,
    pre_ref,
    entry_ref,
    out_ref,
    column_ref,
    row_ref,
    spread_ref,
    mix_ref,
    carry_ref,
):
    step = pl.program_id(0)
    heads, tokens = decay_ref.shape
    span = cot_ref.shape[1]
    states = entry_ref.shape[1]
    per_step = heads // pl.num_programs(0)
    head_size = span // per_step
    half = tokens // 2
    both = (((0,), (0,)), ((), ()))
    last = (((1,), (1,)), ((), ()))

    @pl.when(step == 0)
    def _():
        one = lax.broadcasted_iota(jnp.int32, (tokens, tokens), 0)
        two = lax.broadcasted_iota(jnp.int32, (tokens, tokens), 1)
        cum = jnp.dot(
            decay_ref[...],
            (one <= two).astype(f32),
            precision=lax.Precision.HIGHEST,
            preferred_element_type=f32,
        )
        column_ref[...] = jnp.zeros_like(column_ref)
        column_ref[:, :heads] = lax.dot_general(
            (one >= two).astype(f32),
            decay_ref[...],
            last,
            precision=lax.Precision.HIGHEST,
            preferred_element_type=f32,
        )
        row_ref[...] = cum - jnp.log(step_ref[...])
        grown = jnp.exp(cum)
        shrunk = jnp.exp(cum[:, tokens - 1 :] - cum) * step_ref[...]
        for k, value in enumerate((grown, shrunk)):
            high = value.astype(bf16)
            spread_ref[2 * k] = high
            spread_ref[2 * k + 1] = (value - high.astype(f32)).astype(bf16)
        mix_ref[...] = jnp.zeros_like(mix_ref)
        carry_ref[...] = jnp.zeros_like(carry_ref)

    owner = lax.broadcasted_iota(jnp.int32, (heads, span), 0) * head_size - step * span
    lane = lax.broadcasted_iota(jnp.int32, (heads, span), 1)
    hot = jnp.where((lane >= owner) & (lane < owner + head_size), 1.0, 0.0).astype(bf16)

    def expanded(k):
        scale = lax.dot_general(spread_ref[2 * k], hot, both, preferred_element_type=f32)
        return scale + lax.dot_general(
            spread_ref[2 * k + 1], hot, both, preferred_element_type=f32
        )

    at = pl.multiple_of(step * span, 128)
    out_ref[:, pl.ds(at, span)] = (in_ref[...].astype(f32) * expanded(1)).astype(bf16)
    weighted_cot = (cot_ref[...].astype(f32) * expanded(0)).astype(bf16)
    carry_ref[...] += jnp.dot(weighted_cot, entry_ref[...], preferred_element_type=f32)

    columns = pltpu.roll(column_ref[...], lax.rem(128 - per_step * step, 128), 1)
    rows = [row_ref[pl.ds(per_step * step + j, 1), :] for j in range(per_step)]
    low = lax.broadcasted_iota(jnp.int32, (half, 2 * head_size), 1) < head_size
    later = lax.broadcasted_iota(jnp.int32, (half, half), 0) >= lax.broadcasted_iota(
        jnp.int32, (half, half), 1
    )
    for s, t in ((0, 0), (1, 0), (1, 1)):
        total = mix_ref[s * half : (s + 1) * half, t * half : (t + 1) * half]
        for j in range(per_step):
            lanes = slice(j // 2 * 2 * head_size, (j // 2 + 1) * 2 * head_size)
            left = cot_ref[s * half : (s + 1) * half, lanes]
            keep = low if j % 2 == 0 else jnp.logical_not(low)
            left = jnp.where(keep, left.astype(f32), 0.0).astype(bf16)
            right = in_ref[t * half : (t + 1) * half, lanes]
            scores = lax.dot_general(left, right, last, preferred_element_type=f32)
            gap = columns[s * half : (s + 1) * half, j : j + 1] - rows[j][
                :, t * half : (t + 1) * half
            ]
            if s == t:
                gap = jnp.where(later, gap, -1e30)
            total += scores * jnp.exp(gap)
        mix_ref[s * half : (s + 1) * half, t * half : (t + 1) * half] = total

    @pl.when(step == pl.num_programs(0) - 1)
    def _():
        value = pre_ref[...].astype(f32)
        active = (value / (1.0 + jnp.exp(-value))).astype(bf16)
        mixed = mix_ref[...].astype(bf16)
        inner = lax.dot_general(mixed, active[:, states:], both, preferred_element_type=f32)
        read = carry_ref[...] + jnp.dot(mixed, active[:, :states], preferred_element_type=f32)
        slope = silu_slope(value)
        parts = []
        for part in (inner, slope[:, :states]):
            high = part.astype(bf16)
            parts += [high, (part - high.astype(f32)).astype(bf16)]
        parts.append((read * slope[:, states:]).astype(bf16))
        at = out_ref.shape[1] - len(parts) * states
        for k, part in enumerate(parts):
            out_ref[:, at + k * states : at + (k + 1) * states] = part


def inner_terms(cots, ins, decays, steps, pre, entry):
    tokens, channels = cots.shape
    heads = decays.shape[0]
    states = entry.shape[1]
    grid = 4
    span = channels // grid
    whole = lambda i: (0, 0)
    return pl.pallas_call(
        inner_body,
        grid=(grid,),
        in_specs=[
            pl.BlockSpec((tokens, span), lambda i: (0, i)),
            pl.BlockSpec((tokens, span), lambda i: (0, i)),
            pl.BlockSpec((heads, tokens), whole),
            pl.BlockSpec((heads, tokens), whole),
            pl.BlockSpec((tokens, 2 * states), whole),
            pl.BlockSpec((span, states), lambda i: (i, 0)),
        ],
        out_specs=pl.BlockSpec(memory_space=pltpu.VMEM),
        out_shape=pltpu.VMEM((tokens, channels + 5 * states), bf16),
        scratch_shapes=[
            pltpu.VMEM((tokens, 128), f32),
            pltpu.VMEM((heads, tokens), f32),
            pltpu.VMEM((4, heads, tokens), bf16),
            pltpu.VMEM((tokens, tokens), f32),
            pltpu.VMEM((tokens, states), f32),
        ],
        compiler_params=budget(16),
        cost_estimate=pl.CostEstimate(
            flops=4 * 10**9, transcendentals=2 * 10**6, bytes_accessed=6 * 10**6
        ),
        name="inner_terms",
    )(cots, ins, decays, steps, pre, entry)


def turn_body(in_ref, own_ref, other_ref, hot_ref, turned_ref):
    n_x, _, part, _ = own_ref.shape
    span = in_ref.shape[1]
    n_z, n_c = lax.axis_size("dp_0"), lax.axis_size("dp_1")
    n_y = span // (n_x * part)
    own = part // (n_y * n_z)

    @pl.when(pl.program_id(0) == 0)
    def _():
        row = lax.broadcasted_iota(jnp.int32, (span, 1), 0)
        i, row = lax.rem(row, own), lax.div(row, own)
        z, row = lax.rem(row, n_z), lax.div(row, n_z)
        y, row = lax.rem(row, n_y), lax.div(row, n_y)
        x, c = lax.rem(row, n_x), lax.div(row, n_x)
        source = (((y * n_x + x) * n_z + z) * n_c + c) * own + i
        lane = lax.broadcasted_iota(jnp.int32, (span, span), 1)
        hot_ref[...] = jnp.where(lane == source, 1.0, 0.0).astype(bf16)

    turned_ref[...] = lax.dot_general(
        hot_ref[...], in_ref[...], (((1,), (1,)), ((), ())), preferred_element_type=f32
    ).astype(bf16)
    mine = lax.axis_index("dp_1")
    for x in range(n_x):
        at = pl.multiple_of((mine * n_x + x) * part, 16)
        own_ref[x, 0] = turned_ref[pl.ds(at, part), :]
        at = pl.multiple_of(((1 - mine) * n_x + x) * part, 16)
        other_ref[x, 0] = turned_ref[pl.ds(at, part), :]


def turn(rows_in, n_x, n_c):
    tokens, width = rows_in.shape
    grid = 4
    span = width // grid
    part = span // (n_x * n_c)
    block = pl.BlockSpec((n_x, 1, part, tokens), lambda i: (0, i, 0, 0))
    shape = (n_x, grid, part, tokens)
    own, other = pl.pallas_call(
        turn_body,
        grid=(grid,),
        in_specs=[pl.BlockSpec((tokens, span), lambda i: (0, i))],
        out_specs=[block, block],
        out_shape=[pltpu.VMEM(shape, bf16), pltpu.VMEM(shape, bf16)],
        scratch_shapes=[pltpu.VMEM((span, span), bf16), pltpu.VMEM((span, tokens), bf16)],
        compiler_params=budget(12),
        cost_estimate=pl.CostEstimate(
            flops=10**9, transcendentals=0, bytes_accessed=3 * 10**6
        ),
        name="turn",
    )(rows_in)
    return own.reshape(width // n_c, tokens), other.reshape(width // n_c, tokens)


def finish_body(terms_ref, beyond_ref, peak_ref, grad_ref, send_ref):
    channels, states = beyond_ref.shape
    tokens = terms_ref.shape[0]
    carried = jnp.dot(terms_ref[:, :channels], beyond_ref[...], preferred_element_type=f32)

    def part(k):
        return terms_ref[:, channels + k * states : channels + (k + 1) * states]

    def whole(k):
        return part(k).astype(f32) + part(k + 1).astype(f32)

    send_ref[:tokens, :states] = ((whole(0) + carried) * whole(2)).astype(bf16)
    send_ref[:tokens, states:] = part(4)
    send_ref[tokens:, :states] = jnp.broadcast_to(peak_ref[...], (8, states)).astype(bf16)
    send_ref[tokens:, states:] = jnp.zeros((8, states), bf16)
    grad_ref[...] = send_ref[:tokens, :]


def finish(terms, beyond, peak):
    tokens = terms.shape[0]
    states = beyond.shape[1]
    return pl.pallas_call(
        finish_body,
        out_shape=[
            jax.ShapeDtypeStruct((tokens, 2 * states), bf16),
            jax.ShapeDtypeStruct((tokens + 8, 2 * states), bf16),
        ],
        compiler_params=budget(16),
        name="finish",
    )(terms, beyond, peak)


def product_body(own_ref, mine_ref, other_ref, got_ref, half_ref, peak_ref, held_ref, sem):
    tokens = own_ref.shape[1]
    copy = pltpu.make_async_copy(other_ref, held_ref, sem)
    copy.start()
    total = jnp.dot(own_ref[...], mine_ref[:tokens, :], preferred_element_type=f32)
    copy.wait()
    total += jnp.dot(held_ref[...], got_ref[:tokens, :], preferred_element_type=f32)
    half_ref[...] = total.astype(bf16)
    peak_ref[...] = jnp.maximum(
        mine_ref[tokens:, :].astype(f32), got_ref[tokens:, :].astype(f32)
    )


def multiply(own, mine, other, got):
    rows = own.shape[0]
    cols = mine.shape[1]
    return pl.pallas_call(
        product_body,
        out_shape=[
            jax.ShapeDtypeStruct((rows, cols), bf16),
            jax.ShapeDtypeStruct((8, cols), f32),
        ],
        in_specs=[
            pl.BlockSpec(memory_space=pltpu.VMEM),
            pl.BlockSpec(memory_space=pltpu.VMEM),
            pl.BlockSpec(memory_space=pl.ANY),
            pl.BlockSpec(memory_space=pltpu.VMEM),
        ],
        scratch_shapes=[pltpu.VMEM(other.shape, bf16), pltpu.SemaphoreType.DMA],
        compiler_params=budget(16),
        name="multiply",
    )(own, mine, other, got)


def split_body(got_ref, peak_ref, out_ref, sum_ref):
    count, rows, cols = got_ref.shape
    pieces = out_ref.shape[0]
    own = rows // pieces
    total = got_ref[0].astype(f32)
    for k in range(1, count):
        total += got_ref[k].astype(f32)
    sum_ref[:rows] = total
    sum_ref[rows:] = jnp.zeros((8, cols), f32)
    row = lax.broadcasted_iota(jnp.int32, (8, cols), 0)
    peak = peak_ref[...]
    for q in range(pieces):
        out_ref[q] = jnp.where(row < own, sum_ref[own * q : own * q + 8, :], peak).astype(bf16)


def add_split(got, peak, pieces):
    _, rows, cols = got.shape
    return pl.pallas_call(
        split_body,
        out_shape=jax.ShapeDtypeStruct((pieces, 8, cols), bf16),
        scratch_shapes=[pltpu.VMEM((rows + 8, cols), f32)],
        compiler_params=budget(6),
        name="add_split",
    )(got, peak)


def close_body(got_ref, out_ref):
    count, rows, cols = got_ref.shape
    own = out_ref.shape[0]
    total = got_ref[0].astype(f32)
    for k in range(1, count):
        total += got_ref[k].astype(f32)
    peak = jnp.zeros((rows, cols), f32)
    n_z = lax.axis_size("dp_0")
    at = lax.axis_index("seq_0") * n_z
    pair = lax.axis_size("dp_1")
    spot = (lax.axis_index("dp_0") * pair + lax.axis_index("dp_1")) * own
    for z in range(n_z):
        peak = jnp.maximum(peak, got_ref[at + z].astype(f32))
    lane = lax.broadcasted_iota(jnp.int32, (rows, cols), 1)
    row = lax.broadcasted_iota(jnp.int32, (rows, cols), 0)
    line = jnp.broadcast_to(peak[own : own + 1, :], (rows, cols))
    column = jnp.sum(jnp.where(lane == spot + row, line, 0.0), axis=1, keepdims=True)
    out_ref[...] = (total * (1.0 / (column + epsilon)))[:own]


def close(got, own):
    cols = got.shape[2]
    return pl.pallas_call(
        close_body,
        out_shape=jax.ShapeDtypeStruct((own, cols), f32),
        compiler_params=budget(4),
        name="close",
    )(got)


def on_device(
    layer_input, scan_input, scan_cotangent, step_size, log_decay, state_inputs, entry_state
):
    _, tokens, width = layer_input.shape
    heads = step_size.shape[1]
    channels = scan_input.shape[2]
    head_size = channels // heads
    states = state_inputs.shape[2] // 2
    n_y, n_x, n_z, n_c = (lax.axis_size(a) for a in SEQ_DP)
    n_seq = n_y * n_x
    slice_rows = channels // n_seq
    own_rows = width // (n_seq * n_z * n_c)

    rows_in = layer_input.reshape(tokens, width)
    flat_cot = scan_cotangent.reshape(tokens, channels)
    flat_pre = state_inputs.reshape(tokens, 2 * states)
    decays = log_decay.reshape(heads, tokens)
    sent = summarize(rows_in, flat_cot, decays, flat_pre, n_seq, states)
    got = exchange(sent, SEQ)
    slices, seq_peaks = scan_states(got, slice_rows, head_size)
    beyond = exchange(slices, SEQ).reshape(channels, states)

    terms = inner_terms(
        flat_cot,
        scan_input.reshape(tokens, channels),
        decays,
        step_size.reshape(heads, tokens),
        flat_pre,
        entry_state.reshape(channels, states),
    )
    kept, given = turn(rows_in, n_x, n_c)
    taken = swapped(given)
    state_input_grad, sums = finish(terms, beyond, seq_peaks)
    half, peaks = multiply(kept, sums, taken, swapped(sums))
    quarter = exchange(half.reshape(n_x, width // (n_x * n_c), 2 * states), "seq_1")
    pieces = add_split(quarter, peaks, n_y * n_z)
    arrived = exchange(pieces, ("seq_0", "dp_0"))
    return state_input_grad[None], close(arrived, own_rows)


def solution(mesh):
    torus = Mesh(mesh.devices.reshape(8, 4, 8, 2), SEQ_DP)
    placed = (
        P(DP, SEQ, None),
        P(DP, SEQ, None),
        P(DP, SEQ, None),
        P(DP, None, SEQ),
        P(DP, None, SEQ),
        P(DP, SEQ, None),
        P(DP, SEQ, None, None),
    )
    return jax.shard_map(
        on_device,
        mesh=torus,
        in_specs=placed,
        out_specs=(P(DP, SEQ, None), P(SEQ_DP, None)),
        check_vma=False,
    )
```

```python
import functools

import jax
import jax.numpy as jnp
from jax import lax
from jax.experimental import pallas as pl
from jax.experimental.pallas import tpu as pltpu
from jax.sharding import Mesh
from jax.sharding import PartitionSpec as P

SEQ = ("seq_0", "seq_1")
DP = ("dp_0", "dp_1")
SEQ_DP = SEQ + DP

epsilon = 1e-06
f32 = jnp.float32
bf16 = jnp.bfloat16


def silu_slope(value):
    sigma = 1.0 / (1.0 + jnp.exp(-value))
    return sigma * (1.0 + value * (1.0 - sigma))


def budget(mib):
    return pltpu.CompilerParams(vmem_limit_bytes=mib * 2**20)


def exchange(x, axes):
    return lax.all_to_all(x, axes, 0, 0, tiled=True)


def swapped(x):
    return lax.ppermute(x, "dp_1", [(0, 1), (1, 0)])


def scan_body(head_size, got_ref, out_ref, peak_ref):
    blocks, _, states = got_ref.shape
    rows = out_ref.shape[1]
    slot = lax.axis_index("seq_0") * lax.axis_size("seq_1") + lax.axis_index("seq_1")
    bound = head_size - lax.rem(slot * rows, head_size)
    first = lax.broadcasted_iota(jnp.int32, (rows, states), 0) < bound
    state = jnp.zeros((rows, states), f32)
    peak = jnp.zeros((1, states), f32)
    for k in reversed(range(blocks)):
        out_ref[k] = state.astype(bf16)
        extra = got_ref[k, rows : rows + 8, :].astype(f32)
        peak = jnp.maximum(peak, extra[4:5])
        total = jnp.where(first, extra[0:1] + extra[1:2], extra[2:3] + extra[3:4])
        state = got_ref[k, :rows, :].astype(f32) + total * state
    peak_ref[...] = peak


def scan_states(got, rows, head_size):
    blocks, _, states = got.shape
    return pl.pallas_call(
        functools.partial(scan_body, head_size),
        out_shape=[
            pltpu.VMEM((blocks, rows, states), bf16),
            jax.ShapeDtypeStruct((1, states), f32),
        ],
        compiler_params=budget(8),
        name="scan_states",
    )(got)


def summary_body(in_ref, cot_ref, decay_ref, pre_ref, sent_ref, reads_ref, spread_ref):
    step = pl.program_id(0)
    heads, tokens = decay_ref.shape
    total, rows_all, states = sent_ref.shape
    chunks = total // pl.num_programs(0)
    span = cot_ref.shape[1]
    rows = span // chunks
    head_size = span * pl.num_programs(0) // heads

    @pl.when(step == 0)
    def _():
        below = lax.broadcasted_iota(jnp.int32, (tokens, tokens), 0)
        above = lax.broadcasted_iota(jnp.int32, (tokens, tokens), 1)
        cum = jnp.dot(
            decay_ref[...],
            (below <= above).astype(f32),
            precision=lax.Precision.HIGHEST,
            preferred_element_type=f32,
        )
        grown = jnp.exp(cum)
        high = grown.astype(bf16)
        spread_ref[0] = high
        spread_ref[1] = (grown - high.astype(f32)).astype(bf16)
        value = pre_ref[:, states:].astype(f32)
        reads_ref[...] = (value / (1.0 + jnp.exp(-value))).astype(bf16)

    owner = lax.broadcasted_iota(jnp.int32, (heads, span), 0) * head_size - step * span
    lane = lax.broadcasted_iota(jnp.int32, (heads, span), 1)
    hot = jnp.where((lane >= owner) & (lane < owner + head_size), 1.0, 0.0).astype(bf16)
    both = (((0,), (0,)), ((), ()))
    scale = lax.dot_general(spread_ref[0], hot, both, preferred_element_type=f32)
    scale += lax.dot_general(spread_ref[1], hot, both, preferred_element_type=f32)
    weighted = (cot_ref[...].astype(f32) * scale).astype(bf16)
    later = lax.dot_general(weighted, reads_ref[...], both, preferred_element_type=f32)
    later = later.astype(bf16)
    peak = jnp.max(jnp.abs(in_ref[...]).astype(f32), axis=0, keepdims=True)
    peak = jnp.broadcast_to(peak, (8, span))
    last = scale[tokens - 1 :, :]
    row = lax.broadcasted_iota(jnp.int32, (rows_all - rows, states), 0)
    for d in range(chunks):
        sent_ref[step * chunks + d, :rows, :] = later[d * rows : (d + 1) * rows]
        first = jnp.broadcast_to(last[:, d * rows : d * rows + 1], (8, states))
        second = jnp.broadcast_to(last[:, (d + 1) * rows - 1 : (d + 1) * rows], (8, states))
        first_high = first.astype(bf16).astype(f32)
        second_high = second.astype(bf16).astype(f32)
        turned = pltpu.roll(peak, span - d * rows, 1) if d else peak
        extra = jnp.where(row == 0, first_high, first - first_high)
        extra = jnp.where(row == 2, second_high, extra)
        extra = jnp.where(row == 3, second - second_high, extra)
        extra = jnp.where(row >= 4, turned[:, :states], extra)
        sent_ref[step * chunks + d, rows:, :] = extra.astype(bf16)


def summarize(rows_in, cots, decays, pre, n_seq, head_states):
    tokens, channels = cots.shape
    heads = decays.shape[0]
    states = head_states
    grid = 2
    span = channels // grid
    rows = channels // n_seq
    return pl.pallas_call(
        summary_body,
        grid=(grid,),
        in_specs=[
            pl.BlockSpec((tokens, span), lambda i: (0, i)),
            pl.BlockSpec((tokens, span), lambda i: (0, i)),
            pl.BlockSpec((heads, tokens), lambda i: (0, 0)),
            pl.BlockSpec((tokens, 2 * states), lambda i: (0, 0)),
        ],
        out_specs=pl.BlockSpec(memory_space=pltpu.VMEM),
        out_shape=pltpu.VMEM((n_seq, rows + 8, states), bf16),
        scratch_shapes=[
            pltpu.VMEM((tokens, states), bf16),
            pltpu.VMEM((2, heads, tokens), bf16),
        ],
        compiler_params=budget(60),
        name="summarize",
    )(rows_in, cots, decays, pre)


def inner_body(
    cot_ref,
    in_ref,
    decay_ref,
    step_ref,
    pre_ref,
    entry_ref,
    out_ref,
    column_ref,
    row_ref,
    spread_ref,
    mix_ref,
    carry_ref,
):
    step = pl.program_id(0)
    heads, tokens = decay_ref.shape
    span = cot_ref.shape[1]
    states = entry_ref.shape[1]
    per_step = heads // pl.num_programs(0)
    head_size = span // per_step
    half = tokens // 2
    both = (((0,), (0,)), ((), ()))
    last = (((1,), (1,)), ((), ()))

    @pl.when(step == 0)
    def _():
        one = lax.broadcasted_iota(jnp.int32, (tokens, tokens), 0)
        two = lax.broadcasted_iota(jnp.int32, (tokens, tokens), 1)
        cum = jnp.dot(
            decay_ref[...],
            (one <= two).astype(f32),
            precision=lax.Precision.HIGHEST,
            preferred_element_type=f32,
        )
        column_ref[...] = jnp.zeros_like(column_ref)
        column_ref[:, :heads] = lax.dot_general(
            (one >= two).astype(f32),
            decay_ref[...],
            last,
            precision=lax.Precision.HIGHEST,
            preferred_element_type=f32,
        )
        row_ref[...] = cum - jnp.log(step_ref[...])
        grown = jnp.exp(cum)
        shrunk = jnp.exp(cum[:, tokens - 1 :] - cum) * step_ref[...]
        for k, value in enumerate((grown, shrunk)):
            high = value.astype(bf16)
            spread_ref[2 * k] = high
            spread_ref[2 * k + 1] = (value - high.astype(f32)).astype(bf16)
        mix_ref[...] = jnp.zeros_like(mix_ref)
        carry_ref[...] = jnp.zeros_like(carry_ref)

    owner = lax.broadcasted_iota(jnp.int32, (heads, span), 0) * head_size - step * span
    lane = lax.broadcasted_iota(jnp.int32, (heads, span), 1)
    hot = jnp.where((lane >= owner) & (lane < owner + head_size), 1.0, 0.0).astype(bf16)

    def expanded(k):
        scale = lax.dot_general(spread_ref[2 * k], hot, both, preferred_element_type=f32)
        return scale + lax.dot_general(
            spread_ref[2 * k + 1], hot, both, preferred_element_type=f32
        )

    at = pl.multiple_of(step * span, 128)
    out_ref[:, pl.ds(at, span)] = (in_ref[...].astype(f32) * expanded(1)).astype(bf16)
    weighted_cot = (cot_ref[...].astype(f32) * expanded(0)).astype(bf16)
    carry_ref[...] += jnp.dot(weighted_cot, entry_ref[...], preferred_element_type=f32)

    columns = pltpu.roll(column_ref[...], lax.rem(128 - per_step * step, 128), 1)
    rows = [row_ref[pl.ds(per_step * step + j, 1), :] for j in range(per_step)]
    low = lax.broadcasted_iota(jnp.int32, (half, 2 * head_size), 1) < head_size
    later = lax.broadcasted_iota(jnp.int32, (half, half), 0) >= lax.broadcasted_iota(
        jnp.int32, (half, half), 1
    )
    for s, t in ((0, 0), (1, 0), (1, 1)):
        total = mix_ref[s * half : (s + 1) * half, t * half : (t + 1) * half]
        for j in range(per_step):
            lanes = slice(j // 2 * 2 * head_size, (j // 2 + 1) * 2 * head_size)
            left = cot_ref[s * half : (s + 1) * half, lanes]
            keep = low if j % 2 == 0 else jnp.logical_not(low)
            left = jnp.where(keep, left.astype(f32), 0.0).astype(bf16)
            right = in_ref[t * half : (t + 1) * half, lanes]
            scores = lax.dot_general(left, right, last, preferred_element_type=f32)
            gap = columns[s * half : (s + 1) * half, j : j + 1] - rows[j][
                :, t * half : (t + 1) * half
            ]
            if s == t:
                gap = jnp.where(later, gap, -1e30)
            total += scores * jnp.exp(gap)
        mix_ref[s * half : (s + 1) * half, t * half : (t + 1) * half] = total

    @pl.when(step == pl.num_programs(0) - 1)
    def _():
        value = pre_ref[...].astype(f32)
        active = (value / (1.0 + jnp.exp(-value))).astype(bf16)
        mixed = mix_ref[...].astype(bf16)
        inner = lax.dot_general(mixed, active[:, states:], both, preferred_element_type=f32)
        read = carry_ref[...] + jnp.dot(mixed, active[:, :states], preferred_element_type=f32)
        slope = silu_slope(value)
        parts = []
        for part in (inner, slope[:, :states]):
            high = part.astype(bf16)
            parts += [high, (part - high.astype(f32)).astype(bf16)]
        parts.append((read * slope[:, states:]).astype(bf16))
        at = out_ref.shape[1] - len(parts) * states
        for k, part in enumerate(parts):
            out_ref[:, at + k * states : at + (k + 1) * states] = part


def inner_terms(cots, ins, decays, steps, pre, entry):
    tokens, channels = cots.shape
    heads = decays.shape[0]
    states = entry.shape[1]
    grid = 4
    span = channels // grid
    whole = lambda i: (0, 0)
    return pl.pallas_call(
        inner_body,
        grid=(grid,),
        in_specs=[
            pl.BlockSpec((tokens, span), lambda i: (0, i)),
            pl.BlockSpec((tokens, span), lambda i: (0, i)),
            pl.BlockSpec((heads, tokens), whole),
            pl.BlockSpec((heads, tokens), whole),
            pl.BlockSpec((tokens, 2 * states), whole),
            pl.BlockSpec((span, states), lambda i: (i, 0)),
        ],
        out_specs=pl.BlockSpec(memory_space=pltpu.VMEM),
        out_shape=pltpu.VMEM((tokens, channels + 5 * states), bf16),
        scratch_shapes=[
            pltpu.VMEM((tokens, 128), f32),
            pltpu.VMEM((heads, tokens), f32),
            pltpu.VMEM((4, heads, tokens), bf16),
            pltpu.VMEM((tokens, tokens), f32),
            pltpu.VMEM((tokens, states), f32),
        ],
        compiler_params=budget(16),
        cost_estimate=pl.CostEstimate(
            flops=4 * 10**9, transcendentals=2 * 10**6, bytes_accessed=6 * 10**6
        ),
        name="inner_terms",
    )(cots, ins, decays, steps, pre, entry)


def turn_body(in_ref, own_ref, other_ref, hot_ref, turned_ref):
    n_x, _, part, _ = own_ref.shape
    span = in_ref.shape[1]
    n_z, n_c = lax.axis_size("dp_0"), lax.axis_size("dp_1")
    n_y = span // (n_x * part)
    own = part // (n_y * n_z)

    @pl.when(pl.program_id(0) == 0)
    def _():
        row = lax.broadcasted_iota(jnp.int32, (span, 1), 0)
        i, row = lax.rem(row, own), lax.div(row, own)
        z, row = lax.rem(row, n_z), lax.div(row, n_z)
        y, row = lax.rem(row, n_y), lax.div(row, n_y)
        x, c = lax.rem(row, n_x), lax.div(row, n_x)
        source = (((y * n_x + x) * n_z + z) * n_c + c) * own + i
        lane = lax.broadcasted_iota(jnp.int32, (span, span), 1)
        hot_ref[...] = jnp.where(lane == source, 1.0, 0.0).astype(bf16)

    turned_ref[...] = lax.dot_general(
        hot_ref[...], in_ref[...], (((1,), (1,)), ((), ())), preferred_element_type=f32
    ).astype(bf16)
    mine = lax.axis_index("dp_1")
    for x in range(n_x):
        at = pl.multiple_of((mine * n_x + x) * part, 16)
        own_ref[x, 0] = turned_ref[pl.ds(at, part), :]
        at = pl.multiple_of(((1 - mine) * n_x + x) * part, 16)
        other_ref[x, 0] = turned_ref[pl.ds(at, part), :]


def turn(rows_in, n_x, n_c):
    tokens, width = rows_in.shape
    grid = 4
    span = width // grid
    part = span // (n_x * n_c)
    block = pl.BlockSpec((n_x, 1, part, tokens), lambda i: (0, i, 0, 0))
    shape = (n_x, grid, part, tokens)
    own, other = pl.pallas_call(
        turn_body,
        grid=(grid,),
        in_specs=[pl.BlockSpec((tokens, span), lambda i: (0, i))],
        out_specs=[block, block],
        out_shape=[pltpu.VMEM(shape, bf16), pltpu.VMEM(shape, bf16)],
        scratch_shapes=[pltpu.VMEM((span, span), bf16), pltpu.VMEM((span, tokens), bf16)],
        compiler_params=budget(12),
        cost_estimate=pl.CostEstimate(
            flops=10**9, transcendentals=0, bytes_accessed=3 * 10**6
        ),
        name="turn",
    )(rows_in)
    return own.reshape(width // n_c, tokens), other.reshape(width // n_c, tokens)


def finish_body(terms_ref, beyond_ref, peak_ref, grad_ref, send_ref):
    channels, states = beyond_ref.shape
    tokens = terms_ref.shape[0]
    carried = jnp.dot(terms_ref[:, :channels], beyond_ref[...], preferred_element_type=f32)

    def part(k):
        return terms_ref[:, channels + k * states : channels + (k + 1) * states]

    def whole(k):
        return part(k).astype(f32) + part(k + 1).astype(f32)

    send_ref[:tokens, :states] = ((whole(0) + carried) * whole(2)).astype(bf16)
    send_ref[:tokens, states:] = part(4)
    send_ref[tokens:, :states] = jnp.broadcast_to(peak_ref[...], (8, states)).astype(bf16)
    send_ref[tokens:, states:] = jnp.zeros((8, states), bf16)
    grad_ref[...] = send_ref[:tokens, :]


def finish(terms, beyond, peak):
    tokens = terms.shape[0]
    states = beyond.shape[1]
    return pl.pallas_call(
        finish_body,
        out_shape=[
            jax.ShapeDtypeStruct((tokens, 2 * states), bf16),
            jax.ShapeDtypeStruct((tokens + 8, 2 * states), bf16),
        ],
        compiler_params=budget(16),
        name="finish",
    )(terms, beyond, peak)


def own_body(left_ref, right_ref, out_ref):
    tokens = left_ref.shape[1]
    out_ref[...] = jnp.dot(left_ref[...], right_ref[:tokens, :], preferred_element_type=f32)


def own_product(left, right):
    rows = left.shape[0]
    cols = right.shape[1]
    return pl.pallas_call(
        own_body,
        out_shape=pltpu.VMEM((rows, cols), f32),
        compiler_params=budget(16),
        cost_estimate=pl.CostEstimate(
            flops=3 * 10**8, transcendentals=0, bytes_accessed=2 * 10**6
        ),
        name="own_product",
    )(left, right)


def product_body(own_ref, mine_ref, other_ref, got_ref, half_ref, peak_ref):
    tokens = other_ref.shape[1]
    total = jnp.dot(other_ref[...], got_ref[:tokens, :], preferred_element_type=f32)
    half_ref[...] = (own_ref[...] + total).astype(bf16)
    peak_ref[...] = jnp.maximum(
        mine_ref[tokens:, :].astype(f32), got_ref[tokens:, :].astype(f32)
    )


def multiply(own, mine, other, got):
    rows, cols = own.shape
    return pl.pallas_call(
        product_body,
        out_shape=[
            jax.ShapeDtypeStruct((rows, cols), bf16),
            jax.ShapeDtypeStruct((8, cols), f32),
        ],
        compiler_params=budget(16),
        name="multiply",
    )(own, mine, other, got)


def split_body(got_ref, peak_ref, out_ref, sum_ref):
    count, rows, cols = got_ref.shape
    pieces = out_ref.shape[0]
    own = rows // pieces
    total = got_ref[0].astype(f32)
    for k in range(1, count):
        total += got_ref[k].astype(f32)
    sum_ref[:rows] = total
    sum_ref[rows:] = jnp.zeros((8, cols), f32)
    row = lax.broadcasted_iota(jnp.int32, (8, cols), 0)
    peak = peak_ref[...]
    for q in range(pieces):
        out_ref[q] = jnp.where(row < own, sum_ref[own * q : own * q + 8, :], peak).astype(bf16)


def add_split(got, peak, pieces):
    _, rows, cols = got.shape
    return pl.pallas_call(
        split_body,
        out_shape=jax.ShapeDtypeStruct((pieces, 8, cols), bf16),
        scratch_shapes=[pltpu.VMEM((rows + 8, cols), f32)],
        compiler_params=budget(6),
        name="add_split",
    )(got, peak)


def close_body(got_ref, out_ref):
    count, rows, cols = got_ref.shape
    own = out_ref.shape[0]
    total = got_ref[0].astype(f32)
    for k in range(1, count):
        total += got_ref[k].astype(f32)
    peak = jnp.zeros((rows, cols), f32)
    n_z = lax.axis_size("dp_0")
    at = lax.axis_index("seq_0") * n_z
    pair = lax.axis_size("dp_1")
    spot = (lax.axis_index("dp_0") * pair + lax.axis_index("dp_1")) * own
    for z in range(n_z):
        peak = jnp.maximum(peak, got_ref[at + z].astype(f32))
    lane = lax.broadcasted_iota(jnp.int32, (rows, cols), 1)
    row = lax.broadcasted_iota(jnp.int32, (rows, cols), 0)
    line = jnp.broadcast_to(peak[own : own + 1, :], (rows, cols))
    column = jnp.sum(jnp.where(lane == spot + row, line, 0.0), axis=1, keepdims=True)
    out_ref[...] = (total * (1.0 / (column + epsilon)))[:own]


def close(got, own):
    cols = got.shape[2]
    return pl.pallas_call(
        close_body,
        out_shape=jax.ShapeDtypeStruct((own, cols), f32),
        compiler_params=budget(4),
        name="close",
    )(got)


def on_device(
    layer_input, scan_input, scan_cotangent, step_size, log_decay, state_inputs, entry_state
):
    _, tokens, width = layer_input.shape
    heads = step_size.shape[1]
    channels = scan_input.shape[2]
    head_size = channels // heads
    states = state_inputs.shape[2] // 2
    n_y, n_x, n_z, n_c = (lax.axis_size(a) for a in SEQ_DP)
    n_seq = n_y * n_x
    slice_rows = channels // n_seq
    own_rows = width // (n_seq * n_z * n_c)

    rows_in = layer_input.reshape(tokens, width)
    flat_cot = scan_cotangent.reshape(tokens, channels)
    flat_pre = state_inputs.reshape(tokens, 2 * states)
    decays = log_decay.reshape(heads, tokens)
    sent = summarize(rows_in, flat_cot, decays, flat_pre, n_seq, states)
    got = exchange(sent, SEQ)
    slices, seq_peaks = scan_states(got, slice_rows, head_size)
    beyond = exchange(slices, SEQ).reshape(channels, states)

    terms = inner_terms(
        flat_cot,
        scan_input.reshape(tokens, channels),
        decays,
        step_size.reshape(heads, tokens),
        flat_pre,
        entry_state.reshape(channels, states),
    )
    kept, given = turn(rows_in, n_x, n_c)
    taken = swapped(given)
    state_input_grad, sums = finish(terms, beyond, seq_peaks)
    half, peaks = multiply(own_product(kept, sums), sums, taken, swapped(sums))
    quarter = exchange(half.reshape(n_x, width // (n_x * n_c), 2 * states), "seq_1")
    pieces = add_split(quarter, peaks, n_y * n_z)
    arrived = exchange(pieces, ("seq_0", "dp_0"))
    return state_input_grad[None], close(arrived, own_rows)


def solution(mesh):
    torus = Mesh(mesh.devices.reshape(8, 4, 8, 2), SEQ_DP)
    placed = (
        P(DP, SEQ, None),
        P(DP, SEQ, None),
        P(DP, SEQ, None),
        P(DP, None, SEQ),
        P(DP, None, SEQ),
        P(DP, SEQ, None),
        P(DP, SEQ, None, None),
    )
    return jax.shard_map(
        on_device,
        mesh=torus,
        in_specs=placed,
        out_specs=(P(DP, SEQ, None), P(SEQ_DP, None)),
        check_vma=False,
    )
```

```python
import functools

import jax
import jax.numpy as jnp
from jax import lax
from jax.experimental import pallas as pl
from jax.experimental.pallas import tpu as pltpu
from jax.sharding import Mesh
from jax.sharding import PartitionSpec as P

SEQ = ("seq_0", "seq_1")
DP = ("dp_0", "dp_1")
SEQ_DP = SEQ + DP

epsilon = 1e-06
f32 = jnp.float32
bf16 = jnp.bfloat16


def silu_slope(value):
    sigma = 1.0 / (1.0 + jnp.exp(-value))
    return sigma * (1.0 + value * (1.0 - sigma))


def budget(mib):
    return pltpu.CompilerParams(vmem_limit_bytes=mib * 2**20)


def exchange(x, axes):
    return lax.all_to_all(x, axes, 0, 0, tiled=True)


def swapped(x):
    return lax.ppermute(x, "dp_1", [(0, 1), (1, 0)])


def scan_body(head_size, got_ref, out_ref, peak_ref):
    blocks, _, states = got_ref.shape
    rows = out_ref.shape[1]
    slot = lax.axis_index("seq_0") * lax.axis_size("seq_1") + lax.axis_index("seq_1")
    bound = head_size - lax.rem(slot * rows, head_size)
    first = lax.broadcasted_iota(jnp.int32, (rows, states), 0) < bound
    state = jnp.zeros((rows, states), f32)
    peak = jnp.zeros((1, states), f32)
    for k in reversed(range(blocks)):
        out_ref[k] = state.astype(bf16)
        extra = got_ref[k, rows : rows + 8, :].astype(f32)
        peak = jnp.maximum(peak, extra[4:5])
        total = jnp.where(first, extra[0:1] + extra[1:2], extra[2:3] + extra[3:4])
        state = got_ref[k, :rows, :].astype(f32) + total * state
    peak_ref[...] = peak


def scan_states(got, rows, head_size):
    blocks, _, states = got.shape
    return pl.pallas_call(
        functools.partial(scan_body, head_size),
        out_shape=[
            pltpu.VMEM((blocks, rows, states), bf16),
            jax.ShapeDtypeStruct((1, states), f32),
        ],
        compiler_params=budget(8),
        name="scan_states",
    )(got)


def summary_body(in_ref, cot_ref, decay_ref, pre_ref, sent_ref, reads_ref, spread_ref):
    step = pl.program_id(0)
    heads, tokens = decay_ref.shape
    total, rows_all, states = sent_ref.shape
    chunks = total // pl.num_programs(0)
    span = cot_ref.shape[1]
    rows = span // chunks
    head_size = span * pl.num_programs(0) // heads
    half = spread_ref.shape[0] // 2

    @pl.when(step == 0)
    def _():
        below = lax.broadcasted_iota(jnp.int32, (tokens, tokens), 0)
        above = lax.broadcasted_iota(jnp.int32, (tokens, tokens), 1)
        cum = jnp.dot(
            decay_ref[...],
            (below <= above).astype(f32),
            precision=lax.Precision.HIGHEST,
            preferred_element_type=f32,
        )
        grown = jnp.exp(cum)
        high = grown.astype(bf16)
        spread_ref[...] = jnp.zeros_like(spread_ref)
        spread_ref[:heads] = high
        spread_ref[half : half + heads] = (grown - high.astype(f32)).astype(bf16)
        value = pre_ref[:, states:].astype(f32)
        reads_ref[...] = (value / (1.0 + jnp.exp(-value))).astype(bf16)

    head = lax.broadcasted_iota(jnp.int32, (2 * half, span), 0)
    owner = jnp.where(head < half, head, head - half) * head_size - step * span
    lane = lax.broadcasted_iota(jnp.int32, (2 * half, span), 1)
    hot = jnp.where((lane >= owner) & (lane < owner + head_size), 1.0, 0.0).astype(bf16)
    both = (((0,), (0,)), ((), ()))
    scale = lax.dot_general(spread_ref[...], hot, both, preferred_element_type=f32)
    weighted = (cot_ref[...].astype(f32) * scale).astype(bf16)
    later = lax.dot_general(weighted, reads_ref[...], both, preferred_element_type=f32)
    later = later.astype(bf16)
    peak = jnp.max(jnp.abs(in_ref[...]).astype(f32), axis=0, keepdims=True)
    peak = jnp.broadcast_to(peak, (8, span))
    last = scale[tokens - 1 :, :]
    row = lax.broadcasted_iota(jnp.int32, (rows_all - rows, states), 0)
    for d in range(chunks):
        sent_ref[step * chunks + d, :rows, :] = later[d * rows : (d + 1) * rows]
        first = jnp.broadcast_to(last[:, d * rows : d * rows + 1], (8, states))
        second = jnp.broadcast_to(last[:, (d + 1) * rows - 1 : (d + 1) * rows], (8, states))
        first_high = first.astype(bf16).astype(f32)
        second_high = second.astype(bf16).astype(f32)
        turned = pltpu.roll(peak, span - d * rows, 1) if d else peak
        extra = jnp.where(row == 0, first_high, first - first_high)
        extra = jnp.where(row == 2, second_high, extra)
        extra = jnp.where(row == 3, second - second_high, extra)
        extra = jnp.where(row >= 4, turned[:, :states], extra)
        sent_ref[step * chunks + d, rows:, :] = extra.astype(bf16)


def summarize(rows_in, cots, decays, pre, n_seq, head_states):
    tokens, channels = cots.shape
    heads = decays.shape[0]
    states = head_states
    grid = 2
    span = channels // grid
    rows = channels // n_seq
    return pl.pallas_call(
        summary_body,
        grid=(grid,),
        in_specs=[
            pl.BlockSpec((tokens, span), lambda i: (0, i)),
            pl.BlockSpec((tokens, span), lambda i: (0, i)),
            pl.BlockSpec((heads, tokens), lambda i: (0, 0)),
            pl.BlockSpec((tokens, 2 * states), lambda i: (0, 0)),
        ],
        out_specs=pl.BlockSpec(memory_space=pltpu.VMEM),
        out_shape=pltpu.VMEM((n_seq, rows + 8, states), bf16),
        scratch_shapes=[
            pltpu.VMEM((tokens, states), bf16),
            pltpu.VMEM((2 * (-(-heads // 16) * 16), tokens), bf16),
        ],
        compiler_params=budget(60),
        name="summarize",
    )(rows_in, cots, decays, pre)


def inner_body(
    cot_ref,
    in_ref,
    decay_ref,
    step_ref,
    pre_ref,
    entry_ref,
    out_ref,
    column_ref,
    row_ref,
    spread_ref,
    mix_ref,
    carry_ref,
):
    step = pl.program_id(0)
    heads, tokens = decay_ref.shape
    span = cot_ref.shape[1]
    states = entry_ref.shape[1]
    per_step = heads // pl.num_programs(0)
    head_size = span // per_step
    half = tokens // 2
    both = (((0,), (0,)), ((), ()))
    last = (((1,), (1,)), ((), ()))

    @pl.when(step == 0)
    def _():
        one = lax.broadcasted_iota(jnp.int32, (tokens, tokens), 0)
        two = lax.broadcasted_iota(jnp.int32, (tokens, tokens), 1)
        cum = jnp.dot(
            decay_ref[...],
            (one <= two).astype(f32),
            precision=lax.Precision.HIGHEST,
            preferred_element_type=f32,
        )
        column_ref[...] = jnp.zeros_like(column_ref)
        column_ref[:, :heads] = lax.dot_general(
            (one >= two).astype(f32),
            decay_ref[...],
            last,
            precision=lax.Precision.HIGHEST,
            preferred_element_type=f32,
        )
        row_ref[...] = cum - jnp.log(step_ref[...])
        grown = jnp.exp(cum)
        shrunk = jnp.exp(cum[:, tokens - 1 :] - cum) * step_ref[...]
        for k, value in enumerate((grown, shrunk)):
            high = value.astype(bf16)
            spread_ref[2 * k] = high
            spread_ref[2 * k + 1] = (value - high.astype(f32)).astype(bf16)
        mix_ref[...] = jnp.zeros_like(mix_ref)
        carry_ref[...] = jnp.zeros_like(carry_ref)

    owner = lax.broadcasted_iota(jnp.int32, (heads, span), 0) * head_size - step * span
    lane = lax.broadcasted_iota(jnp.int32, (heads, span), 1)
    hot = jnp.where((lane >= owner) & (lane < owner + head_size), 1.0, 0.0).astype(bf16)

    def expanded(k):
        scale = lax.dot_general(spread_ref[2 * k], hot, both, preferred_element_type=f32)
        return scale + lax.dot_general(
            spread_ref[2 * k + 1], hot, both, preferred_element_type=f32
        )

    at = pl.multiple_of(step * span, 128)
    out_ref[:, pl.ds(at, span)] = (in_ref[...].astype(f32) * expanded(1)).astype(bf16)
    weighted_cot = (cot_ref[...].astype(f32) * expanded(0)).astype(bf16)
    carry_ref[...] += jnp.dot(weighted_cot, entry_ref[...], preferred_element_type=f32)

    columns = pltpu.roll(column_ref[...], lax.rem(128 - per_step * step, 128), 1)
    rows = [row_ref[pl.ds(per_step * step + j, 1), :] for j in range(per_step)]
    low = lax.broadcasted_iota(jnp.int32, (half, 2 * head_size), 1) < head_size
    later = lax.broadcasted_iota(jnp.int32, (half, half), 0) >= lax.broadcasted_iota(
        jnp.int32, (half, half), 1
    )
    for s, t in ((0, 0), (1, 0), (1, 1)):
        total = mix_ref[s * half : (s + 1) * half, t * half : (t + 1) * half]
        for j in range(per_step):
            lanes = slice(j // 2 * 2 * head_size, (j // 2 + 1) * 2 * head_size)
            left = cot_ref[s * half : (s + 1) * half, lanes]
            keep = low if j % 2 == 0 else jnp.logical_not(low)
            left = jnp.where(keep, left.astype(f32), 0.0).astype(bf16)
            right = in_ref[t * half : (t + 1) * half, lanes]
            scores = lax.dot_general(left, right, last, preferred_element_type=f32)
            gap = columns[s * half : (s + 1) * half, j : j + 1] - rows[j][
                :, t * half : (t + 1) * half
            ]
            if s == t:
                gap = jnp.where(later, gap, -1e30)
            total += scores * jnp.exp(gap)
        mix_ref[s * half : (s + 1) * half, t * half : (t + 1) * half] = total

    @pl.when(step == pl.num_programs(0) - 1)
    def _():
        value = pre_ref[...].astype(f32)
        active = (value / (1.0 + jnp.exp(-value))).astype(bf16)
        mixed = mix_ref[...].astype(bf16)
        inner = lax.dot_general(mixed, active[:, states:], both, preferred_element_type=f32)
        read = carry_ref[...] + jnp.dot(mixed, active[:, :states], preferred_element_type=f32)
        slope = silu_slope(value)
        parts = []
        for part in (inner, slope[:, :states]):
            high = part.astype(bf16)
            parts += [high, (part - high.astype(f32)).astype(bf16)]
        parts.append((read * slope[:, states:]).astype(bf16))
        at = out_ref.shape[1] - len(parts) * states
        for k, part in enumerate(parts):
            out_ref[:, at + k * states : at + (k + 1) * states] = part


def inner_terms(cots, ins, decays, steps, pre, entry):
    tokens, channels = cots.shape
    heads = decays.shape[0]
    states = entry.shape[1]
    grid = 4
    span = channels // grid
    whole = lambda i: (0, 0)
    return pl.pallas_call(
        inner_body,
        grid=(grid,),
        in_specs=[
            pl.BlockSpec((tokens, span), lambda i: (0, i)),
            pl.BlockSpec((tokens, span), lambda i: (0, i)),
            pl.BlockSpec((heads, tokens), whole),
            pl.BlockSpec((heads, tokens), whole),
            pl.BlockSpec((tokens, 2 * states), whole),
            pl.BlockSpec((span, states), lambda i: (i, 0)),
        ],
        out_specs=pl.BlockSpec(memory_space=pltpu.VMEM),
        out_shape=pltpu.VMEM((tokens, channels + 5 * states), bf16),
        scratch_shapes=[
            pltpu.VMEM((tokens, 128), f32),
            pltpu.VMEM((heads, tokens), f32),
            pltpu.VMEM((4, heads, tokens), bf16),
            pltpu.VMEM((tokens, tokens), f32),
            pltpu.VMEM((tokens, states), f32),
        ],
        compiler_params=budget(16),
        cost_estimate=pl.CostEstimate(
            flops=4 * 10**9, transcendentals=2 * 10**6, bytes_accessed=6 * 10**6
        ),
        name="inner_terms",
    )(cots, ins, decays, steps, pre, entry)


def turn_body(in_ref, own_ref, other_ref, hot_ref, turned_ref):
    n_x, _, part, _ = own_ref.shape
    span = in_ref.shape[1]
    n_z, n_c = lax.axis_size("dp_0"), lax.axis_size("dp_1")
    n_y = span // (n_x * part)
    own = part // (n_y * n_z)

    @pl.when(pl.program_id(0) == 0)
    def _():
        row = lax.broadcasted_iota(jnp.int32, (span, 1), 0)
        i, row = lax.rem(row, own), lax.div(row, own)
        z, row = lax.rem(row, n_z), lax.div(row, n_z)
        y, row = lax.rem(row, n_y), lax.div(row, n_y)
        x, c = lax.rem(row, n_x), lax.div(row, n_x)
        source = (((y * n_x + x) * n_z + z) * n_c + c) * own + i
        lane = lax.broadcasted_iota(jnp.int32, (span, span), 1)
        hot_ref[...] = jnp.where(lane == source, 1.0, 0.0).astype(bf16)

    turned_ref[...] = lax.dot_general(
        hot_ref[...], in_ref[...], (((1,), (1,)), ((), ())), preferred_element_type=f32
    ).astype(bf16)
    mine = lax.axis_index("dp_1")
    for x in range(n_x):
        at = pl.multiple_of((mine * n_x + x) * part, 16)
        own_ref[x, 0] = turned_ref[pl.ds(at, part), :]
        at = pl.multiple_of(((1 - mine) * n_x + x) * part, 16)
        other_ref[x, 0] = turned_ref[pl.ds(at, part), :]


def turn(rows_in, n_x, n_c):
    tokens, width = rows_in.shape
    grid = 4
    span = width // grid
    part = span // (n_x * n_c)
    block = pl.BlockSpec((n_x, 1, part, tokens), lambda i: (0, i, 0, 0))
    shape = (n_x, grid, part, tokens)
    own, other = pl.pallas_call(
        turn_body,
        grid=(grid,),
        in_specs=[pl.BlockSpec((tokens, span), lambda i: (0, i))],
        out_specs=[block, block],
        out_shape=[pltpu.VMEM(shape, bf16), pltpu.VMEM(shape, bf16)],
        scratch_shapes=[pltpu.VMEM((span, span), bf16), pltpu.VMEM((span, tokens), bf16)],
        compiler_params=budget(12),
        cost_estimate=pl.CostEstimate(
            flops=10**9, transcendentals=0, bytes_accessed=3 * 10**6
        ),
        name="turn",
    )(rows_in)
    return own.reshape(width // n_c, tokens), other.reshape(width // n_c, tokens)


def finish_body(terms_ref, beyond_ref, peak_ref, grad_ref, send_ref):
    channels, states = beyond_ref.shape
    tokens = terms_ref.shape[0]
    carried = jnp.dot(terms_ref[:, :channels], beyond_ref[...], preferred_element_type=f32)

    def part(k):
        return terms_ref[:, channels + k * states : channels + (k + 1) * states]

    def whole(k):
        return part(k).astype(f32) + part(k + 1).astype(f32)

    send_ref[:tokens, :states] = ((whole(0) + carried) * whole(2)).astype(bf16)
    send_ref[:tokens, states:] = part(4)
    send_ref[tokens:, :states] = jnp.broadcast_to(peak_ref[...], (8, states)).astype(bf16)
    send_ref[tokens:, states:] = jnp.zeros((8, states), bf16)
    grad_ref[...] = send_ref[:tokens, :]


def finish(terms, beyond, peak):
    tokens = terms.shape[0]
    states = beyond.shape[1]
    return pl.pallas_call(
        finish_body,
        out_shape=[
            jax.ShapeDtypeStruct((tokens, 2 * states), bf16),
            jax.ShapeDtypeStruct((tokens + 8, 2 * states), bf16),
        ],
        compiler_params=budget(16),
        name="finish",
    )(terms, beyond, peak)


def own_body(left_ref, right_ref, taken_ref, out_ref, held_ref, sem):
    tokens = left_ref.shape[1]
    copy = pltpu.make_async_copy(taken_ref, held_ref, sem)
    copy.start()
    out_ref[...] = jnp.dot(left_ref[...], right_ref[:tokens, :], preferred_element_type=f32)
    copy.wait()


def own_product(left, right, taken):
    rows = left.shape[0]
    cols = right.shape[1]
    return pl.pallas_call(
        own_body,
        in_specs=[
            pl.BlockSpec(memory_space=pltpu.VMEM),
            pl.BlockSpec(memory_space=pltpu.VMEM),
            pl.BlockSpec(memory_space=pltpu.HBM),
        ],
        out_shape=[pltpu.VMEM((rows, cols), f32), pltpu.VMEM(taken.shape, bf16)],
        scratch_shapes=[pltpu.SemaphoreType.DMA],
        compiler_params=budget(16),
        cost_estimate=pl.CostEstimate(
            flops=3 * 10**8, transcendentals=0, bytes_accessed=2 * 10**6
        ),
        name="own_product",
    )(left, right, taken)


def product_body(own_ref, mine_ref, other_ref, got_ref, half_ref, peak_ref):
    tokens = other_ref.shape[1]
    total = jnp.dot(other_ref[...], got_ref[:tokens, :], preferred_element_type=f32)
    half_ref[...] = (own_ref[...] + total).astype(bf16)
    peak_ref[...] = jnp.maximum(
        mine_ref[tokens:, :].astype(f32), got_ref[tokens:, :].astype(f32)
    )


def multiply(own, mine, other, got):
    rows, cols = own.shape
    return pl.pallas_call(
        product_body,
        out_shape=[
            jax.ShapeDtypeStruct((rows, cols), bf16),
            jax.ShapeDtypeStruct((8, cols), f32),
        ],
        compiler_params=budget(16),
        name="multiply",
    )(own, mine, other, got)


def split_body(got_ref, peak_ref, out_ref, sum_ref):
    count, rows, cols = got_ref.shape
    pieces = out_ref.shape[0]
    own = rows // pieces
    total = got_ref[0].astype(f32)
    for k in range(1, count):
        total += got_ref[k].astype(f32)
    sum_ref[:rows] = total
    sum_ref[rows:] = jnp.zeros((8, cols), f32)
    row = lax.broadcasted_iota(jnp.int32, (8, cols), 0)
    peak = peak_ref[...]
    for q in range(pieces):
        out_ref[q] = jnp.where(row < own, sum_ref[own * q : own * q + 8, :], peak).astype(bf16)


def add_split(got, peak, pieces):
    _, rows, cols = got.shape
    return pl.pallas_call(
        split_body,
        out_shape=jax.ShapeDtypeStruct((pieces, 8, cols), bf16),
        scratch_shapes=[pltpu.VMEM((rows + 8, cols), f32)],
        compiler_params=budget(6),
        name="add_split",
    )(got, peak)


def close_body(got_ref, out_ref):
    count, rows, cols = got_ref.shape
    own = out_ref.shape[0]
    total = got_ref[0].astype(f32)
    for k in range(1, count):
        total += got_ref[k].astype(f32)
    peak = jnp.zeros((rows, cols), f32)
    n_z = lax.axis_size("dp_0")
    at = lax.axis_index("seq_0") * n_z
    pair = lax.axis_size("dp_1")
    spot = (lax.axis_index("dp_0") * pair + lax.axis_index("dp_1")) * own
    for z in range(n_z):
        peak = jnp.maximum(peak, got_ref[at + z].astype(f32))
    lane = lax.broadcasted_iota(jnp.int32, (rows, cols), 1)
    row = lax.broadcasted_iota(jnp.int32, (rows, cols), 0)
    line = jnp.broadcast_to(peak[own : own + 1, :], (rows, cols))
    column = jnp.sum(jnp.where(lane == spot + row, line, 0.0), axis=1, keepdims=True)
    out_ref[...] = (total * (1.0 / (column + epsilon)))[:own]


def close(got, own):
    cols = got.shape[2]
    return pl.pallas_call(
        close_body,
        out_shape=jax.ShapeDtypeStruct((own, cols), f32),
        compiler_params=budget(4),
        name="close",
    )(got)


def on_device(
    layer_input, scan_input, scan_cotangent, step_size, log_decay, state_inputs, entry_state
):
    _, tokens, width = layer_input.shape
    heads = step_size.shape[1]
    channels = scan_input.shape[2]
    head_size = channels // heads
    states = state_inputs.shape[2] // 2
    n_y, n_x, n_z, n_c = (lax.axis_size(a) for a in SEQ_DP)
    n_seq = n_y * n_x
    slice_rows = channels // n_seq
    own_rows = width // (n_seq * n_z * n_c)

    rows_in = layer_input.reshape(tokens, width)
    flat_cot = scan_cotangent.reshape(tokens, channels)
    flat_pre = state_inputs.reshape(tokens, 2 * states)
    decays = log_decay.reshape(heads, tokens)
    sent = summarize(rows_in, flat_cot, decays, flat_pre, n_seq, states)
    got = exchange(sent, SEQ)
    slices, seq_peaks = scan_states(got, slice_rows, head_size)
    beyond = exchange(slices, SEQ).reshape(channels, states)

    terms = inner_terms(
        flat_cot,
        scan_input.reshape(tokens, channels),
        decays,
        step_size.reshape(heads, tokens),
        flat_pre,
        entry_state.reshape(channels, states),
    )
    kept, given = turn(rows_in, n_x, n_c)
    taken = swapped(given)
    state_input_grad, sums = finish(terms, beyond, seq_peaks)
    own, held = own_product(kept, sums, taken)
    half, peaks = multiply(own, sums, held, swapped(sums))
    quarter = exchange(half.reshape(n_x, width // (n_x * n_c), 2 * states), "seq_1")
    pieces = add_split(quarter, peaks, n_y * n_z)
    arrived = exchange(pieces, ("seq_0", "dp_0"))
    return state_input_grad[None], close(arrived, own_rows)


def solution(mesh):
    torus = Mesh(mesh.devices.reshape(8, 4, 8, 2), SEQ_DP)
    placed = (
        P(DP, SEQ, None),
        P(DP, SEQ, None),
        P(DP, SEQ, None),
        P(DP, None, SEQ),
        P(DP, None, SEQ),
        P(DP, SEQ, None),
        P(DP, SEQ, None, None),
    )
    return jax.shard_map(
        on_device,
        mesh=torus,
        in_specs=placed,
        out_specs=(P(DP, SEQ, None), P(SEQ_DP, None)),
        check_vma=False,
    )
```

```python
import functools

import jax
import jax.numpy as jnp
from jax import lax
from jax.experimental import pallas as pl
from jax.experimental.pallas import tpu as pltpu
from jax.sharding import Mesh
from jax.sharding import PartitionSpec as P

SEQ = ("seq_0", "seq_1")
DP = ("dp_0", "dp_1")
SEQ_DP = SEQ + DP

epsilon = 1e-06
f32 = jnp.float32
bf16 = jnp.bfloat16


def silu_slope(value):
    sigma = 1.0 / (1.0 + jnp.exp(-value))
    return sigma * (1.0 + value * (1.0 - sigma))


def budget(mib):
    return pltpu.CompilerParams(vmem_limit_bytes=mib * 2**20)


def exchange(x, axes):
    return lax.all_to_all(x, axes, 0, 0, tiled=True)


def swapped(x):
    return lax.ppermute(x, "dp_1", [(0, 1), (1, 0)])


def scan_body(head_size, got_ref, out_ref, peak_ref):
    blocks, _, states = got_ref.shape
    rows = out_ref.shape[1]
    slot = lax.axis_index("seq_0") * lax.axis_size("seq_1") + lax.axis_index("seq_1")
    bound = head_size - lax.rem(slot * rows, head_size)
    first = lax.broadcasted_iota(jnp.int32, (rows, states), 0) < bound
    state = jnp.zeros((rows, states), f32)
    peak = jnp.zeros((1, states), f32)
    for k in reversed(range(blocks)):
        out_ref[k] = state.astype(bf16)
        extra = got_ref[k, rows : rows + 8, :].astype(f32)
        peak = jnp.maximum(peak, extra[4:5])
        total = jnp.where(first, extra[0:1] + extra[1:2], extra[2:3] + extra[3:4])
        state = got_ref[k, :rows, :].astype(f32) + total * state
    peak_ref[...] = peak


def scan_states(got, rows, head_size):
    blocks, _, states = got.shape
    return pl.pallas_call(
        functools.partial(scan_body, head_size),
        out_shape=[
            pltpu.VMEM((blocks, rows, states), bf16),
            jax.ShapeDtypeStruct((1, states), f32),
        ],
        compiler_params=budget(8),
        name="scan_states",
    )(got)


def summary_body(in_ref, cot_ref, decay_ref, pre_ref, sent_ref, reads_ref, spread_ref):
    step = pl.program_id(0)
    heads, tokens = decay_ref.shape
    total, rows_all, states = sent_ref.shape
    chunks = total // pl.num_programs(0)
    span = cot_ref.shape[1]
    rows = span // chunks
    head_size = span * pl.num_programs(0) // heads
    half = spread_ref.shape[0] // 2

    @pl.when(step == 0)
    def _():
        below = lax.broadcasted_iota(jnp.int32, (tokens, tokens), 0)
        above = lax.broadcasted_iota(jnp.int32, (tokens, tokens), 1)
        cum = jnp.dot(
            decay_ref[...],
            (below <= above).astype(f32),
            precision=lax.Precision.HIGHEST,
            preferred_element_type=f32,
        )
        grown = jnp.exp(cum)
        high = grown.astype(bf16)
        spread_ref[...] = jnp.zeros_like(spread_ref)
        spread_ref[:heads] = high
        spread_ref[half : half + heads] = (grown - high.astype(f32)).astype(bf16)
        value = pre_ref[:, states:].astype(f32)
        reads_ref[...] = (value / (1.0 + jnp.exp(-value))).astype(bf16)

    head = lax.broadcasted_iota(jnp.int32, (2 * half, span), 0)
    owner = jnp.where(head < half, head, head - half) * head_size - step * span
    lane = lax.broadcasted_iota(jnp.int32, (2 * half, span), 1)
    hot = jnp.where((lane >= owner) & (lane < owner + head_size), 1.0, 0.0).astype(bf16)
    both = (((0,), (0,)), ((), ()))
    scale = lax.dot_general(spread_ref[...], hot, both, preferred_element_type=f32)
    weighted = (cot_ref[...].astype(f32) * scale).astype(bf16)
    later = lax.dot_general(weighted, reads_ref[...], both, preferred_element_type=f32)
    later = later.astype(bf16)
    peak = jnp.max(jnp.abs(in_ref[...]).astype(f32), axis=0, keepdims=True)
    peak = jnp.broadcast_to(peak, (8, span))
    last = scale[tokens - 1 :, :]
    row = lax.broadcasted_iota(jnp.int32, (rows_all - rows, states), 0)
    for d in range(chunks):
        sent_ref[step * chunks + d, :rows, :] = later[d * rows : (d + 1) * rows]
        first = jnp.broadcast_to(last[:, d * rows : d * rows + 1], (8, states))
        second = jnp.broadcast_to(last[:, (d + 1) * rows - 1 : (d + 1) * rows], (8, states))
        first_high = first.astype(bf16).astype(f32)
        second_high = second.astype(bf16).astype(f32)
        turned = pltpu.roll(peak, span - d * rows, 1) if d else peak
        extra = jnp.where(row == 0, first_high, first - first_high)
        extra = jnp.where(row == 2, second_high, extra)
        extra = jnp.where(row == 3, second - second_high, extra)
        extra = jnp.where(row >= 4, turned[:, :states], extra)
        sent_ref[step * chunks + d, rows:, :] = extra.astype(bf16)


def summarize(rows_in, cots, decays, pre, n_seq, head_states):
    tokens, channels = cots.shape
    heads = decays.shape[0]
    states = head_states
    grid = 2
    span = channels // grid
    rows = channels // n_seq
    return pl.pallas_call(
        summary_body,
        grid=(grid,),
        in_specs=[
            pl.BlockSpec((tokens, span), lambda i: (0, i)),
            pl.BlockSpec((tokens, span), lambda i: (0, i)),
            pl.BlockSpec((heads, tokens), lambda i: (0, 0)),
            pl.BlockSpec((tokens, 2 * states), lambda i: (0, 0)),
        ],
        out_specs=pl.BlockSpec(memory_space=pltpu.VMEM),
        out_shape=pltpu.VMEM((n_seq, rows + 8, states), bf16),
        scratch_shapes=[
            pltpu.VMEM((tokens, states), bf16),
            pltpu.VMEM((2 * (-(-heads // 16) * 16), tokens), bf16),
        ],
        compiler_params=budget(60),
        name="summarize",
    )(rows_in, cots, decays, pre)


def inner_body(
    cot_ref,
    in_ref,
    decay_ref,
    step_ref,
    pre_ref,
    entry_ref,
    out_ref,
    read_ref,
    column_ref,
    row_ref,
    spread_ref,
    mix_ref,
    carry_ref,
):
    step = pl.program_id(0)
    heads, tokens = decay_ref.shape
    span = cot_ref.shape[1]
    states = entry_ref.shape[1]
    per_step = heads // pl.num_programs(0)
    head_size = span // per_step
    half = tokens // 2
    both = (((0,), (0,)), ((), ()))
    last = (((1,), (1,)), ((), ()))

    @pl.when(step == 0)
    def _():
        one = lax.broadcasted_iota(jnp.int32, (tokens, tokens), 0)
        two = lax.broadcasted_iota(jnp.int32, (tokens, tokens), 1)
        cum = jnp.dot(
            decay_ref[...],
            (one <= two).astype(f32),
            precision=lax.Precision.HIGHEST,
            preferred_element_type=f32,
        )
        column_ref[...] = jnp.zeros_like(column_ref)
        column_ref[:, :heads] = lax.dot_general(
            (one >= two).astype(f32),
            decay_ref[...],
            last,
            precision=lax.Precision.HIGHEST,
            preferred_element_type=f32,
        )
        row_ref[...] = cum - jnp.log(step_ref[...])
        grown = jnp.exp(cum)
        shrunk = jnp.exp(cum[:, tokens - 1 :] - cum) * step_ref[...]
        for k, value in enumerate((grown, shrunk)):
            high = value.astype(bf16)
            spread_ref[2 * k] = high
            spread_ref[2 * k + 1] = (value - high.astype(f32)).astype(bf16)
        mix_ref[...] = jnp.zeros_like(mix_ref)
        carry_ref[...] = jnp.zeros_like(carry_ref)

    owner = lax.broadcasted_iota(jnp.int32, (heads, span), 0) * head_size - step * span
    lane = lax.broadcasted_iota(jnp.int32, (heads, span), 1)
    hot = jnp.where((lane >= owner) & (lane < owner + head_size), 1.0, 0.0).astype(bf16)

    def expanded(k):
        scale = lax.dot_general(spread_ref[2 * k], hot, both, preferred_element_type=f32)
        return scale + lax.dot_general(
            spread_ref[2 * k + 1], hot, both, preferred_element_type=f32
        )

    at = pl.multiple_of(step * span, 128)
    out_ref[:, pl.ds(at, span)] = (in_ref[...].astype(f32) * expanded(1)).astype(bf16)
    weighted_cot = (cot_ref[...].astype(f32) * expanded(0)).astype(bf16)
    carry_ref[...] += jnp.dot(weighted_cot, entry_ref[...], preferred_element_type=f32)

    columns = pltpu.roll(column_ref[...], lax.rem(128 - per_step * step, 128), 1)
    rows = [row_ref[pl.ds(per_step * step + j, 1), :] for j in range(per_step)]
    low = lax.broadcasted_iota(jnp.int32, (half, 2 * head_size), 1) < head_size
    later = lax.broadcasted_iota(jnp.int32, (half, half), 0) >= lax.broadcasted_iota(
        jnp.int32, (half, half), 1
    )
    for s, t in ((0, 0), (1, 0), (1, 1)):
        total = mix_ref[s * half : (s + 1) * half, t * half : (t + 1) * half]
        for j in range(per_step):
            lanes = slice(j // 2 * 2 * head_size, (j // 2 + 1) * 2 * head_size)
            left = cot_ref[s * half : (s + 1) * half, lanes]
            keep = low if j % 2 == 0 else jnp.logical_not(low)
            left = jnp.where(keep, left.astype(f32), 0.0).astype(bf16)
            right = in_ref[t * half : (t + 1) * half, lanes]
            scores = lax.dot_general(left, right, last, preferred_element_type=f32)
            gap = columns[s * half : (s + 1) * half, j : j + 1] - rows[j][
                :, t * half : (t + 1) * half
            ]
            if s == t:
                gap = jnp.where(later, gap, -1e30)
            total += scores * jnp.exp(gap)
        mix_ref[s * half : (s + 1) * half, t * half : (t + 1) * half] = total

    @pl.when(step == pl.num_programs(0) - 1)
    def _():
        value = pre_ref[...].astype(f32)
        active = (value / (1.0 + jnp.exp(-value))).astype(bf16)
        mixed = mix_ref[...].astype(bf16)
        inner = lax.dot_general(mixed, active[:, states:], both, preferred_element_type=f32)
        read = carry_ref[...] + jnp.dot(mixed, active[:, :states], preferred_element_type=f32)
        slope = silu_slope(value)
        parts = []
        for part in (inner, slope[:, :states]):
            high = part.astype(bf16)
            parts += [high, (part - high.astype(f32)).astype(bf16)]
        read_ref[...] = (read * slope[:, states:]).astype(bf16)
        at = out_ref.shape[1] - len(parts) * states
        for k, part in enumerate(parts):
            out_ref[:, at + k * states : at + (k + 1) * states] = part


def inner_terms(cots, ins, decays, steps, pre, entry):
    tokens, channels = cots.shape
    heads = decays.shape[0]
    states = entry.shape[1]
    grid = 4
    span = channels // grid
    whole = lambda i: (0, 0)
    return pl.pallas_call(
        inner_body,
        grid=(grid,),
        in_specs=[
            pl.BlockSpec((tokens, span), lambda i: (0, i)),
            pl.BlockSpec((tokens, span), lambda i: (0, i)),
            pl.BlockSpec((heads, tokens), whole),
            pl.BlockSpec((heads, tokens), whole),
            pl.BlockSpec((tokens, 2 * states), whole),
            pl.BlockSpec((span, states), lambda i: (i, 0)),
        ],
        out_specs=[pl.BlockSpec(memory_space=pltpu.VMEM), pl.BlockSpec((tokens, states), whole)],
        out_shape=[
            pltpu.VMEM((tokens, channels + 4 * states), bf16),
            jax.ShapeDtypeStruct((tokens, states), bf16),
        ],
        scratch_shapes=[
            pltpu.VMEM((tokens, 128), f32),
            pltpu.VMEM((heads, tokens), f32),
            pltpu.VMEM((4, heads, tokens), bf16),
            pltpu.VMEM((tokens, tokens), f32),
            pltpu.VMEM((tokens, states), f32),
        ],
        compiler_params=budget(16),
        cost_estimate=pl.CostEstimate(
            flops=4 * 10**9, transcendentals=2 * 10**6, bytes_accessed=6 * 10**6
        ),
        name="inner_terms",
    )(cots, ins, decays, steps, pre, entry)


def turn_body(in_ref, own_ref, other_ref, hot_ref, turned_ref):
    n_x, _, part, _ = own_ref.shape
    span = in_ref.shape[1]
    n_z, n_c = lax.axis_size("dp_0"), lax.axis_size("dp_1")
    n_y = span // (n_x * part)
    own = part // (n_y * n_z)

    @pl.when(pl.program_id(0) == 0)
    def _():
        row = lax.broadcasted_iota(jnp.int32, (span, 1), 0)
        i, row = lax.rem(row, own), lax.div(row, own)
        z, row = lax.rem(row, n_z), lax.div(row, n_z)
        y, row = lax.rem(row, n_y), lax.div(row, n_y)
        x, c = lax.rem(row, n_x), lax.div(row, n_x)
        source = (((y * n_x + x) * n_z + z) * n_c + c) * own + i
        lane = lax.broadcasted_iota(jnp.int32, (span, span), 1)
        hot_ref[...] = jnp.where(lane == source, 1.0, 0.0).astype(bf16)

    turned_ref[...] = lax.dot_general(
        hot_ref[...], in_ref[...], (((1,), (1,)), ((), ())), preferred_element_type=f32
    ).astype(bf16)
    mine = lax.axis_index("dp_1")
    for x in range(n_x):
        at = pl.multiple_of((mine * n_x + x) * part, 16)
        own_ref[x, 0] = turned_ref[pl.ds(at, part), :]
        at = pl.multiple_of(((1 - mine) * n_x + x) * part, 16)
        other_ref[x, 0] = turned_ref[pl.ds(at, part), :]


def turn(rows_in, n_x, n_c):
    tokens, width = rows_in.shape
    grid = 4
    span = width // grid
    part = span // (n_x * n_c)
    block = pl.BlockSpec((n_x, 1, part, tokens), lambda i: (0, i, 0, 0))
    shape = (n_x, grid, part, tokens)
    own, other = pl.pallas_call(
        turn_body,
        grid=(grid,),
        in_specs=[pl.BlockSpec((tokens, span), lambda i: (0, i))],
        out_specs=[block, block],
        out_shape=[pltpu.VMEM(shape, bf16), pltpu.VMEM(shape, bf16)],
        scratch_shapes=[pltpu.VMEM((span, span), bf16), pltpu.VMEM((span, tokens), bf16)],
        compiler_params=budget(12),
        cost_estimate=pl.CostEstimate(
            flops=10**9, transcendentals=0, bytes_accessed=3 * 10**6
        ),
        name="turn",
    )(rows_in)
    return own.reshape(width // n_c, tokens), other.reshape(width // n_c, tokens)


def finish_body(terms_ref, beyond_ref, peak_ref, send_ref):
    channels, states = beyond_ref.shape
    tokens = terms_ref.shape[0]
    carried = jnp.dot(terms_ref[:, :channels], beyond_ref[...], preferred_element_type=f32)

    def part(k):
        return terms_ref[:, channels + k * states : channels + (k + 1) * states]

    def whole(k):
        return part(k).astype(f32) + part(k + 1).astype(f32)

    send_ref[:tokens, :] = ((whole(0) + carried) * whole(2)).astype(bf16)
    send_ref[tokens:, :] = jnp.broadcast_to(peak_ref[...], (8, states)).astype(bf16)


def finish(terms, beyond, peak):
    tokens = terms.shape[0]
    states = beyond.shape[1]
    return pl.pallas_call(
        finish_body,
        out_shape=jax.ShapeDtypeStruct((tokens + 8, states), bf16),
        compiler_params=budget(16),
        name="finish",
    )(terms, beyond, peak)


def early_body(left_ref, mine_ref, other_ref, got_ref, keep_ref, send_ref, total_ref):
    rows = keep_ref.shape[1]
    total_ref[...] = jnp.dot(
        left_ref[...], mine_ref[...], preferred_element_type=f32
    ) + jnp.dot(other_ref[...], got_ref[...], preferred_element_type=f32)
    x = lax.axis_index("seq_1")
    odd, high = lax.rem(x, 2), lax.div(x, 2)
    for j in range(2):
        side = odd + j - 2 * odd * j
        at = pl.multiple_of((2 * high + side) * rows, 8)
        keep_ref[j] = total_ref[pl.ds(at, rows), :]
        at = pl.multiple_of((2 * (1 - high) + side) * rows, 8)
        send_ref[j] = total_ref[pl.ds(at, rows), :].astype(bf16)


def early_product(left, mine, other, got, n_x):
    rows, cols = left.shape[0], mine.shape[1]
    shape = (2, rows // n_x, cols)
    return pl.pallas_call(
        early_body,
        out_shape=[jax.ShapeDtypeStruct(shape, f32), jax.ShapeDtypeStruct(shape, bf16)],
        scratch_shapes=[pltpu.VMEM((rows, cols), f32)],
        compiler_params=budget(16),
        cost_estimate=pl.CostEstimate(
            flops=3 * 10**8, transcendentals=0, bytes_accessed=2 * 10**6
        ),
        name="early_product",
    )(left, mine, other, got)


def first_body(keep_ref, got_ref, rest_ref, send_ref):
    rest_ref[...] = keep_ref[0] + got_ref[0].astype(f32)
    send_ref[...] = (keep_ref[1] + got_ref[1].astype(f32)).astype(bf16)


def add_first(keep, got):
    return pl.pallas_call(
        first_body,
        out_shape=[
            jax.ShapeDtypeStruct(keep.shape[1:], f32),
            jax.ShapeDtypeStruct(keep.shape[1:], bf16),
        ],
        compiler_params=budget(8),
        name="add_first",
    )(keep, got)


def second_body(rest_ref, got_ref, out_ref):
    out_ref[...] = rest_ref[...] + got_ref[...].astype(f32)


def add_second(rest, got):
    return pl.pallas_call(
        second_body,
        out_shape=jax.ShapeDtypeStruct(rest.shape, f32),
        compiler_params=budget(8),
        name="add_second",
    )(rest, got)


def own_body(left_ref, right_ref, taken_ref, read_ref, out_ref, held_ref, grad_ref, sem):
    tokens = left_ref.shape[1]
    copy = pltpu.make_async_copy(taken_ref, held_ref, sem)
    copy.start()
    out_ref[...] = jnp.dot(left_ref[...], right_ref[:tokens, :], preferred_element_type=f32)
    states = read_ref.shape[1]
    grad_ref[:, :states] = right_ref[:tokens, :]
    grad_ref[:, states:] = read_ref[...]
    copy.wait()


def own_product(left, right, taken, read):
    rows = left.shape[0]
    cols = right.shape[1]
    return pl.pallas_call(
        own_body,
        in_specs=[
            pl.BlockSpec(memory_space=pltpu.VMEM),
            pl.BlockSpec(memory_space=pltpu.VMEM),
            pl.BlockSpec(memory_space=pltpu.HBM),
            pl.BlockSpec(memory_space=pltpu.VMEM),
        ],
        out_shape=[
            pltpu.VMEM((rows, cols), f32),
            pltpu.VMEM(taken.shape, bf16),
            jax.ShapeDtypeStruct((left.shape[1], 2 * cols), bf16),
        ],
        scratch_shapes=[pltpu.SemaphoreType.DMA],
        compiler_params=budget(16),
        cost_estimate=pl.CostEstimate(
            flops=3 * 10**8, transcendentals=0, bytes_accessed=2 * 10**6
        ),
        name="own_product",
    )(left, right, taken, read)


def product_body(own_ref, mine_ref, other_ref, got_ref, half_ref, peak_ref):
    tokens = other_ref.shape[1]
    total = jnp.dot(other_ref[...], got_ref[:tokens, :], preferred_element_type=f32)
    half_ref[...] = (own_ref[...] + total).astype(bf16)
    peak_ref[...] = jnp.maximum(
        mine_ref[tokens:, :].astype(f32), got_ref[tokens:, :].astype(f32)
    )


def multiply(own, mine, other, got):
    rows, cols = own.shape
    return pl.pallas_call(
        product_body,
        out_shape=[
            jax.ShapeDtypeStruct((rows, cols), bf16),
            jax.ShapeDtypeStruct((8, cols), f32),
        ],
        compiler_params=budget(16),
        name="multiply",
    )(own, mine, other, got)


def split_body(got_ref, read_ref, peak_ref, out_ref, sum_ref):
    count, rows, states = got_ref.shape
    pieces, _, cols = out_ref.shape
    own = rows // pieces
    total = got_ref[0].astype(f32)
    for k in range(1, count):
        total += got_ref[k].astype(f32)
    sum_ref[:rows, :states] = total
    sum_ref[:rows, states:] = read_ref[...]
    sum_ref[rows:] = jnp.zeros((8, cols), f32)
    row = lax.broadcasted_iota(jnp.int32, (8, cols), 0)
    peak = jnp.concatenate([peak_ref[...], jnp.zeros_like(peak_ref)], axis=1)
    for q in range(pieces):
        out_ref[q] = jnp.where(row < own, sum_ref[own * q : own * q + 8, :], peak).astype(bf16)


def add_split(got, read, peak, pieces):
    _, rows, states = got.shape
    cols = 2 * states
    return pl.pallas_call(
        split_body,
        out_shape=jax.ShapeDtypeStruct((pieces, 8, cols), bf16),
        scratch_shapes=[pltpu.VMEM((rows + 8, cols), f32)],
        compiler_params=budget(6),
        name="add_split",
    )(got, read, peak)


def close_body(got_ref, out_ref):
    count, rows, cols = got_ref.shape
    own = out_ref.shape[0]
    total = got_ref[0].astype(f32)
    for k in range(1, count):
        total += got_ref[k].astype(f32)
    peak = jnp.zeros((rows, cols), f32)
    n_z = lax.axis_size("dp_0")
    at = lax.axis_index("seq_0") * n_z
    pair = lax.axis_size("dp_1")
    spot = (lax.axis_index("dp_0") * pair + lax.axis_index("dp_1")) * own
    for z in range(n_z):
        peak = jnp.maximum(peak, got_ref[at + z].astype(f32))
    lane = lax.broadcasted_iota(jnp.int32, (rows, cols), 1)
    row = lax.broadcasted_iota(jnp.int32, (rows, cols), 0)
    line = jnp.broadcast_to(peak[own : own + 1, :], (rows, cols))
    column = jnp.sum(jnp.where(lane == spot + row, line, 0.0), axis=1, keepdims=True)
    out_ref[...] = (total * (1.0 / (column + epsilon)))[:own]


def close(got, own):
    cols = got.shape[2]
    return pl.pallas_call(
        close_body,
        out_shape=jax.ShapeDtypeStruct((own, cols), f32),
        compiler_params=budget(4),
        name="close",
    )(got)


def on_device(
    layer_input, scan_input, scan_cotangent, step_size, log_decay, state_inputs, entry_state
):
    _, tokens, width = layer_input.shape
    heads = step_size.shape[1]
    channels = scan_input.shape[2]
    head_size = channels // heads
    states = state_inputs.shape[2] // 2
    n_y, n_x, n_z, n_c = (lax.axis_size(a) for a in SEQ_DP)
    n_seq = n_y * n_x
    slice_rows = channels // n_seq
    own_rows = width // (n_seq * n_z * n_c)

    rows_in = layer_input.reshape(tokens, width)
    flat_cot = scan_cotangent.reshape(tokens, channels)
    flat_pre = state_inputs.reshape(tokens, 2 * states)
    decays = log_decay.reshape(heads, tokens)
    sent = summarize(rows_in, flat_cot, decays, flat_pre, n_seq, states)
    got = exchange(sent, SEQ)
    slices, seq_peaks = scan_states(got, slice_rows, head_size)
    beyond = exchange(slices, SEQ).reshape(channels, states)
    kept, given = turn(rows_in, n_x, n_c)
    taken = swapped(given)
    terms, grad_read = inner_terms(
        flat_cot,
        scan_input.reshape(tokens, channels),
        decays,
        step_size.reshape(heads, tokens),
        flat_pre,
        entry_state.reshape(channels, states),
    )
    keep, send = early_product(kept, grad_read, taken, swapped(grad_read), n_x)
    got = lax.ppermute(send, "seq_1", [(i, (i + 2) % 4) for i in range(4)])
    rest, send = add_first(keep, got)
    got = lax.ppermute(send, "seq_1", [(0, 1), (1, 0), (2, 3), (3, 2)])
    read = add_second(rest, got)
    sums = finish(terms, beyond, seq_peaks)
    own, held, state_input_grad = own_product(kept, sums, taken, grad_read)
    half, peaks = multiply(own, sums, held, swapped(sums))
    quarter = exchange(half.reshape(n_x, width // (n_x * n_c), states), "seq_1")
    pieces = add_split(quarter, read, peaks, n_y * n_z)
    arrived = exchange(pieces, ("seq_0", "dp_0"))
    return state_input_grad[None], close(arrived, own_rows)


def solution(mesh):
    torus = Mesh(mesh.devices.reshape(8, 4, 8, 2), SEQ_DP)
    placed = (
        P(DP, SEQ, None),
        P(DP, SEQ, None),
        P(DP, SEQ, None),
        P(DP, None, SEQ),
        P(DP, None, SEQ),
        P(DP, SEQ, None),
        P(DP, SEQ, None, None),
    )

    return jax.shard_map(
        on_device,
        mesh=torus,
        in_specs=placed,
        out_specs=(P(DP, SEQ, None), P(SEQ_DP, None)),
        check_vma=False,
    )
```

```python
import functools

import jax
import jax.numpy as jnp
from jax import lax
from jax.experimental import pallas as pl
from jax.experimental.pallas import tpu as pltpu
from jax.sharding import Mesh
from jax.sharding import PartitionSpec as P

SEQ = ("seq_0", "seq_1")
DP = ("dp_0", "dp_1")
SEQ_DP = SEQ + DP

epsilon = 1e-06
f32 = jnp.float32
bf16 = jnp.bfloat16


def silu_slope(value):
    sigma = 1.0 / (1.0 + jnp.exp(-value))
    return sigma * (1.0 + value * (1.0 - sigma))


def budget(mib):
    return pltpu.CompilerParams(vmem_limit_bytes=mib * 2**20)


def exchange(x, axes):
    return lax.all_to_all(x, axes, 0, 0, tiled=True)


def swapped(x):
    return lax.ppermute(x, "dp_1", [(0, 1), (1, 0)])


def scan_body(head_size, got_ref, out_ref, peak_ref):
    blocks, _, states = got_ref.shape
    rows = out_ref.shape[1]
    slot = lax.axis_index("seq_0") * lax.axis_size("seq_1") + lax.axis_index("seq_1")
    bound = head_size - lax.rem(slot * rows, head_size)
    first = lax.broadcasted_iota(jnp.int32, (rows, states), 0) < bound
    state = jnp.zeros((rows, states), f32)
    peak = jnp.zeros((1, states), f32)
    for k in reversed(range(blocks)):
        out_ref[k] = state.astype(bf16)
        extra = got_ref[k, rows : rows + 8, :].astype(f32)
        peak = jnp.maximum(peak, extra[4:5])
        total = jnp.where(first, extra[0:1] + extra[1:2], extra[2:3] + extra[3:4])
        state = got_ref[k, :rows, :].astype(f32) + total * state
    peak_ref[...] = peak


def scan_states(got, rows, head_size):
    blocks, _, states = got.shape
    return pl.pallas_call(
        functools.partial(scan_body, head_size),
        out_shape=[
            pltpu.VMEM((blocks, rows, states), bf16),
            jax.ShapeDtypeStruct((1, states), f32),
        ],
        compiler_params=budget(8),
        name="scan_states",
    )(got)


def summary_body(in_ref, cot_ref, decay_ref, pre_ref, sent_ref, reads_ref, spread_ref):
    step = pl.program_id(0)
    heads, tokens = decay_ref.shape
    total, rows_all, states = sent_ref.shape
    chunks = total // pl.num_programs(0)
    span = cot_ref.shape[1]
    rows = span // chunks
    head_size = span * pl.num_programs(0) // heads
    half = spread_ref.shape[0] // 2

    @pl.when(step == 0)
    def _():
        below = lax.broadcasted_iota(jnp.int32, (tokens, tokens), 0)
        above = lax.broadcasted_iota(jnp.int32, (tokens, tokens), 1)
        cum = jnp.dot(
            decay_ref[...],
            (below <= above).astype(f32),
            precision=lax.Precision.HIGHEST,
            preferred_element_type=f32,
        )
        grown = jnp.exp(cum)
        high = grown.astype(bf16)
        spread_ref[...] = jnp.zeros_like(spread_ref)
        spread_ref[:heads] = high
        spread_ref[half : half + heads] = (grown - high.astype(f32)).astype(bf16)
        value = pre_ref[:, states:].astype(f32)
        reads_ref[...] = (value / (1.0 + jnp.exp(-value))).astype(bf16)

    head = lax.broadcasted_iota(jnp.int32, (2 * half, span), 0)
    owner = jnp.where(head < half, head, head - half) * head_size - step * span
    lane = lax.broadcasted_iota(jnp.int32, (2 * half, span), 1)
    hot = jnp.where((lane >= owner) & (lane < owner + head_size), 1.0, 0.0).astype(bf16)
    both = (((0,), (0,)), ((), ()))
    scale = lax.dot_general(spread_ref[...], hot, both, preferred_element_type=f32)
    weighted = (cot_ref[...].astype(f32) * scale).astype(bf16)
    later = lax.dot_general(weighted, reads_ref[...], both, preferred_element_type=f32)
    later = later.astype(bf16)
    peak = jnp.max(jnp.abs(in_ref[...]).astype(f32), axis=0, keepdims=True)
    peak = jnp.broadcast_to(peak, (8, span))
    last = scale[tokens - 1 :, :]
    row = lax.broadcasted_iota(jnp.int32, (rows_all - rows, states), 0)
    for d in range(chunks):
        sent_ref[step * chunks + d, :rows, :] = later[d * rows : (d + 1) * rows]
        first = jnp.broadcast_to(last[:, d * rows : d * rows + 1], (8, states))
        second = jnp.broadcast_to(last[:, (d + 1) * rows - 1 : (d + 1) * rows], (8, states))
        first_high = first.astype(bf16).astype(f32)
        second_high = second.astype(bf16).astype(f32)
        turned = pltpu.roll(peak, span - d * rows, 1) if d else peak
        extra = jnp.where(row == 0, first_high, first - first_high)
        extra = jnp.where(row == 2, second_high, extra)
        extra = jnp.where(row == 3, second - second_high, extra)
        extra = jnp.where(row >= 4, turned[:, :states], extra)
        sent_ref[step * chunks + d, rows:, :] = extra.astype(bf16)


def summarize(rows_in, cots, decays, pre, n_seq, head_states):
    tokens, channels = cots.shape
    heads = decays.shape[0]
    states = head_states
    grid = 2
    span = channels // grid
    rows = channels // n_seq
    return pl.pallas_call(
        summary_body,
        grid=(grid,),
        in_specs=[
            pl.BlockSpec((tokens, span), lambda i: (0, i)),
            pl.BlockSpec((tokens, span), lambda i: (0, i)),
            pl.BlockSpec((heads, tokens), lambda i: (0, 0)),
            pl.BlockSpec((tokens, 2 * states), lambda i: (0, 0)),
        ],
        out_specs=pl.BlockSpec(memory_space=pltpu.VMEM),
        out_shape=pltpu.VMEM((n_seq, rows + 8, states), bf16),
        scratch_shapes=[
            pltpu.VMEM((tokens, states), bf16),
            pltpu.VMEM((2 * (-(-heads // 16) * 16), tokens), bf16),
        ],
        compiler_params=budget(60),
        name="summarize",
    )(rows_in, cots, decays, pre)


def inner_body(
    cot_ref,
    in_ref,
    decay_ref,
    step_ref,
    pre_ref,
    entry_ref,
    out_ref,
    column_ref,
    row_ref,
    spread_ref,
    mix_ref,
    carry_ref,
):
    step = pl.program_id(0)
    heads, tokens = decay_ref.shape
    span = cot_ref.shape[1]
    states = entry_ref.shape[1]
    per_step = heads // pl.num_programs(0)
    head_size = span // per_step
    half = tokens // 2
    both = (((0,), (0,)), ((), ()))
    last = (((1,), (1,)), ((), ()))

    @pl.when(step == 0)
    def _():
        one = lax.broadcasted_iota(jnp.int32, (tokens, tokens), 0)
        two = lax.broadcasted_iota(jnp.int32, (tokens, tokens), 1)
        cum = jnp.dot(
            decay_ref[...],
            (one <= two).astype(f32),
            precision=lax.Precision.HIGHEST,
            preferred_element_type=f32,
        )
        column_ref[...] = jnp.zeros_like(column_ref)
        column_ref[:, :heads] = lax.dot_general(
            (one >= two).astype(f32),
            decay_ref[...],
            last,
            precision=lax.Precision.HIGHEST,
            preferred_element_type=f32,
        )
        row_ref[...] = cum - jnp.log(step_ref[...])
        grown = jnp.exp(cum)
        shrunk = jnp.exp(cum[:, tokens - 1 :] - cum) * step_ref[...]
        for k, value in enumerate((grown, shrunk)):
            high = value.astype(bf16)
            spread_ref[2 * k] = high
            spread_ref[2 * k + 1] = (value - high.astype(f32)).astype(bf16)
        mix_ref[...] = jnp.zeros_like(mix_ref)
        carry_ref[...] = jnp.zeros_like(carry_ref)

    owner = lax.broadcasted_iota(jnp.int32, (heads, span), 0) * head_size - step * span
    lane = lax.broadcasted_iota(jnp.int32, (heads, span), 1)
    hot = jnp.where((lane >= owner) & (lane < owner + head_size), 1.0, 0.0).astype(bf16)

    def expanded(k):
        scale = lax.dot_general(spread_ref[2 * k], hot, both, preferred_element_type=f32)
        return scale + lax.dot_general(
            spread_ref[2 * k + 1], hot, both, preferred_element_type=f32
        )

    at = pl.multiple_of(step * span, 128)
    out_ref[:, pl.ds(at, span)] = (in_ref[...].astype(f32) * expanded(1)).astype(bf16)
    weighted_cot = (cot_ref[...].astype(f32) * expanded(0)).astype(bf16)
    carry_ref[...] += jnp.dot(weighted_cot, entry_ref[...], preferred_element_type=f32)

    columns = pltpu.roll(column_ref[...], lax.rem(128 - per_step * step, 128), 1)
    rows = [row_ref[pl.ds(per_step * step + j, 1), :] for j in range(per_step)]
    low = lax.broadcasted_iota(jnp.int32, (half, 2 * head_size), 1) < head_size
    later = lax.broadcasted_iota(jnp.int32, (half, half), 0) >= lax.broadcasted_iota(
        jnp.int32, (half, half), 1
    )
    for s, t in ((0, 0), (1, 0), (1, 1)):
        total = mix_ref[s * half : (s + 1) * half, t * half : (t + 1) * half]
        for j in range(per_step):
            lanes = slice(j // 2 * 2 * head_size, (j // 2 + 1) * 2 * head_size)
            left = cot_ref[s * half : (s + 1) * half, lanes]
            keep = low if j % 2 == 0 else jnp.logical_not(low)
            left = jnp.where(keep, left.astype(f32), 0.0).astype(bf16)
            right = in_ref[t * half : (t + 1) * half, lanes]
            scores = lax.dot_general(left, right, last, preferred_element_type=f32)
            gap = columns[s * half : (s + 1) * half, j : j + 1] - rows[j][
                :, t * half : (t + 1) * half
            ]
            if s == t:
                gap = jnp.where(later, gap, -1e30)
            total += scores * jnp.exp(gap)
        mix_ref[s * half : (s + 1) * half, t * half : (t + 1) * half] = total

    @pl.when(step == pl.num_programs(0) - 1)
    def _():
        value = pre_ref[...].astype(f32)
        active = (value / (1.0 + jnp.exp(-value))).astype(bf16)
        mixed = mix_ref[...].astype(bf16)
        inner = lax.dot_general(mixed, active[:, states:], both, preferred_element_type=f32)
        read = carry_ref[...] + jnp.dot(mixed, active[:, :states], preferred_element_type=f32)
        slope = silu_slope(value)
        parts = []
        for part in (inner, slope[:, :states]):
            high = part.astype(bf16)
            parts += [high, (part - high.astype(f32)).astype(bf16)]
        parts.append((read * slope[:, states:]).astype(bf16))
        at = out_ref.shape[1] - len(parts) * states
        for k, part in enumerate(parts):
            out_ref[:, at + k * states : at + (k + 1) * states] = part


def inner_terms(cots, ins, decays, steps, pre, entry):
    tokens, channels = cots.shape
    heads = decays.shape[0]
    states = entry.shape[1]
    grid = 4
    span = channels // grid
    whole = lambda i: (0, 0)
    return pl.pallas_call(
        inner_body,
        grid=(grid,),
        in_specs=[
            pl.BlockSpec((tokens, span), lambda i: (0, i)),
            pl.BlockSpec((tokens, span), lambda i: (0, i)),
            pl.BlockSpec((heads, tokens), whole),
            pl.BlockSpec((heads, tokens), whole),
            pl.BlockSpec((tokens, 2 * states), whole),
            pl.BlockSpec((span, states), lambda i: (i, 0)),
        ],
        out_specs=pl.BlockSpec(memory_space=pltpu.VMEM),
        out_shape=pltpu.VMEM((tokens, channels + 5 * states), bf16),
        scratch_shapes=[
            pltpu.VMEM((tokens, 128), f32),
            pltpu.VMEM((heads, tokens), f32),
            pltpu.VMEM((4, heads, tokens), bf16),
            pltpu.VMEM((tokens, tokens), f32),
            pltpu.VMEM((tokens, states), f32),
        ],
        compiler_params=budget(16),
        cost_estimate=pl.CostEstimate(
            flops=4 * 10**9, transcendentals=2 * 10**6, bytes_accessed=6 * 10**6
        ),
        name="inner_terms",
    )(cots, ins, decays, steps, pre, entry)


def turn_body(in_ref, own_ref, other_ref, hot_ref, turned_ref):
    n_x, _, part, _ = own_ref.shape
    span = in_ref.shape[1]
    n_z, n_c = lax.axis_size("dp_0"), lax.axis_size("dp_1")
    n_y = span // (n_x * part)
    own = part // (n_y * n_z)

    @pl.when(pl.program_id(0) == 0)
    def _():
        row = lax.broadcasted_iota(jnp.int32, (span, 1), 0)
        i, row = lax.rem(row, own), lax.div(row, own)
        z, row = lax.rem(row, n_z), lax.div(row, n_z)
        y, row = lax.rem(row, n_y), lax.div(row, n_y)
        x, c = lax.rem(row, n_x), lax.div(row, n_x)
        source = (((y * n_x + x) * n_z + z) * n_c + c) * own + i
        lane = lax.broadcasted_iota(jnp.int32, (span, span), 1)
        hot_ref[...] = jnp.where(lane == source, 1.0, 0.0).astype(bf16)

    turned_ref[...] = lax.dot_general(
        hot_ref[...], in_ref[...], (((1,), (1,)), ((), ())), preferred_element_type=f32
    ).astype(bf16)
    mine = lax.axis_index("dp_1")
    for x in range(n_x):
        at = pl.multiple_of((mine * n_x + x) * part, 16)
        own_ref[x, 0] = turned_ref[pl.ds(at, part), :]
        at = pl.multiple_of(((1 - mine) * n_x + x) * part, 16)
        other_ref[x, 0] = turned_ref[pl.ds(at, part), :]


def turn(rows_in, n_x, n_c):
    tokens, width = rows_in.shape
    grid = 4
    span = width // grid
    part = span // (n_x * n_c)
    block = pl.BlockSpec((n_x, 1, part, tokens), lambda i: (0, i, 0, 0))
    shape = (n_x, grid, part, tokens)
    own, other = pl.pallas_call(
        turn_body,
        grid=(grid,),
        in_specs=[pl.BlockSpec((tokens, span), lambda i: (0, i))],
        out_specs=[block, block],
        out_shape=[pltpu.VMEM(shape, bf16), pltpu.VMEM(shape, bf16)],
        scratch_shapes=[pltpu.VMEM((span, span), bf16), pltpu.VMEM((span, tokens), bf16)],
        compiler_params=budget(12),
        cost_estimate=pl.CostEstimate(
            flops=10**9, transcendentals=0, bytes_accessed=3 * 10**6
        ),
        name="turn",
    )(rows_in)
    return own.reshape(width // n_c, tokens), other.reshape(width // n_c, tokens)


def finish_body(terms_ref, beyond_ref, peak_ref, send_ref):
    channels, states = beyond_ref.shape
    tokens = terms_ref.shape[0]
    carried = jnp.dot(terms_ref[:, :channels], beyond_ref[...], preferred_element_type=f32)

    def part(k):
        return terms_ref[:, channels + k * states : channels + (k + 1) * states]

    def whole(k):
        return part(k).astype(f32) + part(k + 1).astype(f32)

    send_ref[:tokens, :states] = ((whole(0) + carried) * whole(2)).astype(bf16)
    send_ref[:tokens, states:] = part(4)
    send_ref[tokens:, :states] = jnp.broadcast_to(peak_ref[...], (8, states)).astype(bf16)
    send_ref[tokens:, states:] = jnp.zeros((8, states), bf16)


def finish(terms, beyond, peak):
    tokens = terms.shape[0]
    states = beyond.shape[1]
    return pl.pallas_call(
        finish_body,
        out_shape=jax.ShapeDtypeStruct((tokens + 8, 2 * states), bf16),
        compiler_params=budget(16),
        name="finish",
    )(terms, beyond, peak)


def own_body(left_ref, right_ref, taken_ref, out_ref, held_ref, grad_ref, sem):
    tokens = left_ref.shape[1]
    copy = pltpu.make_async_copy(taken_ref, held_ref, sem)
    copy.start()
    out_ref[...] = jnp.dot(left_ref[...], right_ref[:tokens, :], preferred_element_type=f32)
    grad_ref[...] = right_ref[:tokens, :]
    copy.wait()


def own_product(left, right, taken):
    rows = left.shape[0]
    cols = right.shape[1]
    return pl.pallas_call(
        own_body,
        in_specs=[
            pl.BlockSpec(memory_space=pltpu.VMEM),
            pl.BlockSpec(memory_space=pltpu.VMEM),
            pl.BlockSpec(memory_space=pltpu.HBM),
        ],
        out_shape=[
            pltpu.VMEM((rows, cols), f32),
            pltpu.VMEM(taken.shape, bf16),
            jax.ShapeDtypeStruct((left.shape[1], cols), bf16),
        ],
        scratch_shapes=[pltpu.SemaphoreType.DMA],
        compiler_params=budget(16),
        cost_estimate=pl.CostEstimate(
            flops=3 * 10**8, transcendentals=0, bytes_accessed=2 * 10**6
        ),
        name="own_product",
    )(left, right, taken)


def product_body(own_ref, mine_ref, other_ref, got_ref, half_ref, peak_ref):
    tokens = other_ref.shape[1]
    total = jnp.dot(other_ref[...], got_ref[:tokens, :], preferred_element_type=f32)
    half_ref[...] = (own_ref[...] + total).astype(bf16)
    peak_ref[...] = jnp.maximum(
        mine_ref[tokens:, :].astype(f32), got_ref[tokens:, :].astype(f32)
    )


def multiply(own, mine, other, got):
    rows, cols = own.shape
    return pl.pallas_call(
        product_body,
        out_shape=[
            jax.ShapeDtypeStruct((rows, cols), bf16),
            jax.ShapeDtypeStruct((8, cols), f32),
        ],
        compiler_params=budget(16),
        name="multiply",
    )(own, mine, other, got)


def split_body(got_ref, peak_ref, out_ref, sum_ref):
    count, rows, cols = got_ref.shape
    pieces = out_ref.shape[0]
    own = rows // pieces
    total = got_ref[0].astype(f32)
    for k in range(1, count):
        total += got_ref[k].astype(f32)
    sum_ref[:rows] = total
    sum_ref[rows:] = jnp.zeros((8, cols), f32)
    row = lax.broadcasted_iota(jnp.int32, (8, cols), 0)
    peak = peak_ref[...]
    for q in range(pieces):
        out_ref[q] = jnp.where(row < own, sum_ref[own * q : own * q + 8, :], peak).astype(bf16)


def add_split(got, peak, pieces):
    _, rows, cols = got.shape
    return pl.pallas_call(
        split_body,
        out_shape=jax.ShapeDtypeStruct((pieces, 8, cols), bf16),
        scratch_shapes=[pltpu.VMEM((rows + 8, cols), f32)],
        compiler_params=budget(6),
        name="add_split",
    )(got, peak)


def close_body(got_ref, out_ref):
    count, rows, cols = got_ref.shape
    own = out_ref.shape[0]
    total = got_ref[0].astype(f32)
    for k in range(1, count):
        total += got_ref[k].astype(f32)
    peak = jnp.zeros((rows, cols), f32)
    n_z = lax.axis_size("dp_0")
    at = lax.axis_index("seq_0") * n_z
    pair = lax.axis_size("dp_1")
    spot = (lax.axis_index("dp_0") * pair + lax.axis_index("dp_1")) * own
    for z in range(n_z):
        peak = jnp.maximum(peak, got_ref[at + z].astype(f32))
    lane = lax.broadcasted_iota(jnp.int32, (rows, cols), 1)
    row = lax.broadcasted_iota(jnp.int32, (rows, cols), 0)
    line = jnp.broadcast_to(peak[own : own + 1, :], (rows, cols))
    column = jnp.sum(jnp.where(lane == spot + row, line, 0.0), axis=1, keepdims=True)
    out_ref[...] = (total * (1.0 / (column + epsilon)))[:own]


def close(got, own):
    cols = got.shape[2]
    return pl.pallas_call(
        close_body,
        out_shape=jax.ShapeDtypeStruct((own, cols), f32),
        compiler_params=budget(4),
        name="close",
    )(got)


def on_device(
    layer_input, scan_input, scan_cotangent, step_size, log_decay, state_inputs, entry_state
):
    _, tokens, width = layer_input.shape
    heads = step_size.shape[1]
    channels = scan_input.shape[2]
    head_size = channels // heads
    states = state_inputs.shape[2] // 2
    n_y, n_x, n_z, n_c = (lax.axis_size(a) for a in SEQ_DP)
    n_seq = n_y * n_x
    slice_rows = channels // n_seq
    own_rows = width // (n_seq * n_z * n_c)

    rows_in = layer_input.reshape(tokens, width)
    flat_cot = scan_cotangent.reshape(tokens, channels)
    flat_pre = state_inputs.reshape(tokens, 2 * states)
    decays = log_decay.reshape(heads, tokens)
    sent = summarize(rows_in, flat_cot, decays, flat_pre, n_seq, states)
    got = exchange(sent, SEQ)
    slices, seq_peaks = scan_states(got, slice_rows, head_size)
    beyond = exchange(slices, SEQ).reshape(channels, states)

    terms = inner_terms(
        flat_cot,
        scan_input.reshape(tokens, channels),
        decays,
        step_size.reshape(heads, tokens),
        flat_pre,
        entry_state.reshape(channels, states),
    )
    kept, given = turn(rows_in, n_x, n_c)
    taken = swapped(given)
    sums = finish(terms, beyond, seq_peaks)
    own, held, state_input_grad = own_product(kept, sums, taken)
    half, peaks = multiply(own, sums, held, swapped(sums))
    quarter = exchange(half.reshape(n_x, width // (n_x * n_c), 2 * states), "seq_1")
    pieces = add_split(quarter, peaks, n_y * n_z)
    arrived = exchange(pieces, ("seq_0", "dp_0"))
    return state_input_grad[None], close(arrived, own_rows)


def solution(mesh):
    torus = Mesh(mesh.devices.reshape(8, 4, 8, 2), SEQ_DP)
    placed = (
        P(DP, SEQ, None),
        P(DP, SEQ, None),
        P(DP, SEQ, None),
        P(DP, None, SEQ),
        P(DP, None, SEQ),
        P(DP, SEQ, None),
        P(DP, SEQ, None, None),
    )
    return jax.shard_map(
        on_device,
        mesh=torus,
        in_specs=placed,
        out_specs=(P(DP, SEQ, None), P(SEQ_DP, None)),
        check_vma=False,
    )
```
